8 devices in a mesh: dp: 1 (over z), tp: 2 (over y), cp: 4 (over x, core).
Axes of the slice: x: 2, y: 2, z: 1, core: 2. Of those that a mesh axis runs over, the one named last changes fastest.
Arguments:
- x: bfloat16 [2048, 4096], P(('dp', 'cp'))
- attn_gain: bfloat16 [4096], replicated
- w_q: bfloat16 [4096, 4096], P(None, 'tp')
- w_k: bfloat16 [4096, 1024], P(None, 'tp')
- w_v: bfloat16 [4096, 1024], P(None, 'tp')
- w_o: bfloat16 [4096, 4096], P('tp')
- mlp_gain: bfloat16 [4096], replicated
- w_gate: bfloat16 [4096, 12288], P(None, 'tp')
- w_up: bfloat16 [4096, 12288], P(None, 'tp')
- w_down: bfloat16 [12288, 4096], P('tp')
Outputs:
- output 1: bfloat16 [2048, 4096], P(('dp', 'cp'))
- output 2: bfloat16 [2048, 8, 128], P(('dp', 'cp'), 'tp')
- output 3: bfloat16 [2048, 8, 128], P(('dp', 'cp'), 'tp')
All inputs are finite; a program needn't handle non-finite values.
Results may differ from the reference program's by a relative error of at most 0.0129251.
Values are sent between devices in bfloat16 or wider.
A program may use at most 1 GiB of HBM per device.

```python
import jax
import jax.numpy as jnp
from jax import lax

SEQ_LEN = 2048
MODEL_DIM = 4096
FF_DIM = 12288
NUM_HEADS = 32
KV_HEADS = 8
HEAD_DIM = 128
ROPE_THETA = 1000000
BLOCK_LEN = 256
NORM_EPS = 1e-5
MASK_VALUE = -1e30


def setup_inputs(seed: int = 0, part: int = 0) -> dict:
    root = jax.random.key(seed)
    key_list = jax.random.split(root, 10)
    seq_key = jax.random.fold_in(key_list[0], part)
    noise_key, dir_key, freq_key, phase_key = jax.random.split(seq_key, 4)
    seq_frac = jnp.arange(SEQ_LEN, dtype=jnp.float32) / SEQ_LEN
    wave_freq = jax.random.uniform(freq_key, (4,), jnp.float32, 0.3, 2.0)
    wave_phase = jax.random.uniform(phase_key, (4,), jnp.float32, 0.0, 6.2831853)
    waves = jnp.cos(6.2831853 * seq_frac[:, None] * wave_freq[None, :] + wave_phase[None, :])
    directions = 0.5 * jax.random.normal(dir_key, (4, MODEL_DIM), jnp.float32)
    noise = jax.random.normal(noise_key, (SEQ_LEN, MODEL_DIM), jnp.float32)
    x = (0.6 * noise + jnp.dot(waves, directions)).astype(jnp.bfloat16)
    q_cols = NUM_HEADS * HEAD_DIM
    kv_cols = KV_HEADS * HEAD_DIM

    def weight(key, rows, cols):
        return (jax.random.normal(key, (rows, cols), jnp.float32) * rows ** -0.5).astype(jnp.bfloat16)

    def gain(key):
        return jax.random.uniform(key, (MODEL_DIM,), jnp.float32, 0.5, 1.5).astype(jnp.bfloat16)

    return {
        'x': x,
        'attn_gain': gain(key_list[1]),
        'w_q': weight(key_list[2], MODEL_DIM, q_cols),
        'w_k': weight(key_list[3], MODEL_DIM, kv_cols),
        'w_v': weight(key_list[4], MODEL_DIM, kv_cols),
        'w_o': weight(key_list[5], q_cols, MODEL_DIM),
        'mlp_gain': gain(key_list[6]),
        'w_gate': weight(key_list[7], MODEL_DIM, FF_DIM),
        'w_up': weight(key_list[8], MODEL_DIM, FF_DIM),
        'w_down': weight(key_list[9], FF_DIM, MODEL_DIM),
    }


def rms_norm(rows, gain):
    wide = rows.astype(jnp.float32)
    inv_rms = lax.rsqrt(jnp.mean(wide * wide, axis=-1, keepdims=True) + NORM_EPS)
    return (wide * inv_rms * gain.astype(jnp.float32)).astype(jnp.bfloat16)


def rope_tables(positions):
    inv_freq = jnp.asarray(ROPE_THETA, jnp.float32) ** (-jnp.arange(0, HEAD_DIM, 2, dtype=jnp.float32) / HEAD_DIM)
    angles = positions.astype(jnp.float32)[:, None] * inv_freq[None, :]
    return jnp.cos(angles), jnp.sin(angles)


def apply_rope(heads, cos_b, sin_b):
    half = HEAD_DIM // 2
    wide = heads.astype(jnp.float32)
    first = wide[..., :half]
    second = wide[..., half:]
    return jnp.concatenate([first * cos_b - second * sin_b, second * cos_b + first * sin_b], axis=-1).astype(jnp.bfloat16)


def causal_attention(queries, keys, values):
    groups = NUM_HEADS // KV_HEADS
    n_blocks = SEQ_LEN // BLOCK_LEN
    q_blocks = queries.reshape(n_blocks, BLOCK_LEN, KV_HEADS, groups, HEAD_DIM)
    k_blocks = keys.reshape(n_blocks, BLOCK_LEN, KV_HEADS, HEAD_DIM)
    v_blocks = values.reshape(n_blocks, BLOCK_LEN, KV_HEADS, HEAD_DIM)
    offsets = jnp.arange(BLOCK_LEN)
    block_ids = jnp.arange(n_blocks)

    def one_query_block(operands):
        q_blk, q_idx = operands
        q_wide = q_blk.astype(jnp.float32)
        q_pos = q_idx * BLOCK_LEN + offsets

        def key_step(carry, inputs):
            run_max, run_sum, weighted = carry
            k_blk, v_blk, k_idx = inputs
            k_pos = k_idx * BLOCK_LEN + offsets
            scores = jnp.einsum('qkgd,skd->kgqs', q_wide, k_blk.astype(jnp.float32)) * (HEAD_DIM ** -0.5)
            scores = jnp.where(k_pos[None, :] <= q_pos[:, None], scores, MASK_VALUE)
            new_max = jnp.maximum(run_max, jnp.max(scores, axis=-1))
            rescale = jnp.exp(run_max - new_max)
            exp_scores = jnp.exp(scores - new_max[..., None])
            new_sum = run_sum * rescale + jnp.sum(exp_scores, axis=-1)
            exp_rounded = exp_scores.astype(jnp.bfloat16).astype(jnp.float32)
            new_weighted = weighted * rescale[..., None] + jnp.einsum('kgqs,skd->kgqd', exp_rounded, v_blk.astype(jnp.float32))
            return (new_max, new_sum, new_weighted), None

        stat_shape = (KV_HEADS, groups, BLOCK_LEN)
        init = (jnp.full(stat_shape, MASK_VALUE, jnp.float32), jnp.zeros(stat_shape, jnp.float32), jnp.zeros(stat_shape + (HEAD_DIM,), jnp.float32))
        final, unused = lax.scan(key_step, init, (k_blocks, v_blocks, block_ids))
        block_out = final[2] / final[1][..., None]
        return jnp.transpose(block_out, (2, 0, 1, 3)).astype(jnp.bfloat16)

    outs = lax.map(one_query_block, (q_blocks, block_ids))
    return outs.reshape(SEQ_LEN, NUM_HEADS * HEAD_DIM)


def reference(x, attn_gain, w_q, w_k, w_v, w_o, mlp_gain, w_gate, w_up, w_down):
    groups = NUM_HEADS // KV_HEADS
    cos_tab, sin_tab = rope_tables(jnp.arange(SEQ_LEN))
    normed = rms_norm(x, attn_gain)
    queries = jnp.dot(normed, w_q, preferred_element_type=jnp.float32).astype(jnp.bfloat16).reshape(SEQ_LEN, NUM_HEADS, HEAD_DIM)
    keys = jnp.dot(normed, w_k, preferred_element_type=jnp.float32).astype(jnp.bfloat16).reshape(SEQ_LEN, KV_HEADS, HEAD_DIM)
    values = jnp.dot(normed, w_v, preferred_element_type=jnp.float32).astype(jnp.bfloat16).reshape(SEQ_LEN, KV_HEADS, HEAD_DIM)
    queries = apply_rope(queries, cos_tab[:, None, :], sin_tab[:, None, :])
    keys = apply_rope(keys, cos_tab[:, None, :], sin_tab[:, None, :])
    attn_rows = causal_attention(queries.reshape(SEQ_LEN, KV_HEADS, groups, HEAD_DIM), keys, values)
    attn_proj = jnp.dot(attn_rows, w_o, preferred_element_type=jnp.float32)
    hidden = (x.astype(jnp.float32) + attn_proj).astype(jnp.bfloat16)
    normed_mlp = rms_norm(hidden, mlp_gain)
    gate_proj = jnp.dot(normed_mlp, w_gate, preferred_element_type=jnp.float32)
    up_proj = jnp.dot(normed_mlp, w_up, preferred_element_type=jnp.float32)
    activated = (jax.nn.silu(gate_proj) * up_proj).astype(jnp.bfloat16)
    down_proj = jnp.dot(activated, w_down, preferred_element_type=jnp.float32)
    x_out = (hidden.astype(jnp.float32) + down_proj).astype(jnp.bfloat16)
    return (x_out, keys, values)
```

```python
import functools
import jax
import jax.numpy as jnp
from jax import lax
from jax.experimental import pallas as pl
from jax.experimental.pallas import tpu as pltpu
from jax.sharding import PartitionSpec as P

HEAD_DIM = 128
ROPE_THETA = 1000000.0
NORM_EPS = 1e-5
MASK_VALUE = -1e30
EXP2_SCALE = HEAD_DIM ** -0.5 * 1.4426950408889634
BF = jnp.bfloat16
F32 = jnp.float32
VMEM_BIG = 60 * 1024 * 1024
ANY = pl.BlockSpec(memory_space=pl.ANY)
SMEM = pl.BlockSpec(memory_space=pltpu.SMEM)


def cost(flops, nbytes):
    return pl.CostEstimate(flops=flops, bytes_accessed=nbytes, transcendentals=0)


def params():
    return pltpu.CompilerParams(vmem_limit_bytes=VMEM_BIG)


def rope_tables(positions):
    inv_freq = jnp.asarray(ROPE_THETA, F32) ** (-jnp.arange(0, HEAD_DIM, 2, dtype=F32) / HEAD_DIM)
    angles = positions.astype(F32)[:, None] * inv_freq[None, :]
    return jnp.cos(angles), jnp.sin(angles)


def norm_rows(rows, gain_row):
    inv_rms = lax.rsqrt(jnp.mean(rows * rows, axis=-1, keepdims=True) + NORM_EPS)
    return (rows * inv_rms * gain_row.astype(F32)).astype(BF)


def rope_block(prod, cos_full, sin_full):
    pieces = []
    for head in range(prod.shape[1] // HEAD_DIM):
        u = prod[:, head * HEAD_DIM:(head + 1) * HEAD_DIM].astype(BF).astype(F32)
        pieces.append((u * cos_full + pltpu.roll(u, HEAD_DIM // 2, 1) * sin_full).astype(BF))
    return jnp.concatenate(pieces, axis=1)


def kv_kernel(x_ref, gain_ref, wk_ref, wv_ref, cos_ref, sin_ref, n_ref, k_ref, v_ref):
    @pl.when(pl.program_id(0) == 0)
    def _():
        def chunk(i, c):
            rows = pl.ds(pl.multiple_of(i * 64, 64), 64)
            n_ref[rows, :] = norm_rows(x_ref[rows, :].astype(F32), gain_ref[...])
            return c
        lax.fori_loop(0, x_ref.shape[0] // 64, chunk, 0)
    n = n_ref[...]
    k = jnp.dot(n, wk_ref[...], preferred_element_type=F32)
    k_ref[...] = rope_block(k, cos_ref[...], sin_ref[...])
    v_ref[...] = jnp.dot(n, wv_ref[...], preferred_element_type=F32).astype(BF)


def kv_proj(x, gain, w_k, w_v, cos_full, sin_full):
    rows, width = x.shape
    cols = w_k.shape[1]
    bn = 256
    whole = lambda a: pl.BlockSpec(a.shape, lambda i: (0, 0))
    wspec = pl.BlockSpec((width, bn), lambda i: (0, i))
    ospec = pl.BlockSpec((rows, bn), lambda i: (0, i))
    return pl.pallas_call(
        kv_kernel, grid=(cols // bn,),
        in_specs=[whole(x), whole(gain), wspec, wspec, whole(cos_full), whole(sin_full)],
        out_specs=[pl.BlockSpec((rows, width), lambda i: (0, 0)), ospec, ospec],
        out_shape=[jax.ShapeDtypeStruct((rows, width), BF), jax.ShapeDtypeStruct((rows, cols), BF), jax.ShapeDtypeStruct((rows, cols), BF)],
        compiler_params=params(), name='kv_proj',
        cost_estimate=cost(4 * rows * width * cols, 2 * 2 * width * (rows + cols)),
    )(x, gain, w_k, w_v, cos_full, sin_full)


def q_kernel(n_ref, w_ref, cos_ref, sin_ref, q_ref):
    prod = jnp.dot(n_ref[...], w_ref[...], preferred_element_type=F32)
    q_ref[...] = rope_block(prod, cos_ref[...], sin_ref[...])


def q_proj(n, w_q, cos_full, sin_full):
    rows, width = n.shape
    cols = w_q.shape[1]
    bn = 512
    whole = lambda a: pl.BlockSpec(a.shape, lambda i: (0, 0))
    return pl.pallas_call(
        q_kernel, grid=(cols // bn,),
        in_specs=[whole(n), pl.BlockSpec((width, bn), lambda i: (0, i)), whole(cos_full), whole(sin_full)],
        out_specs=pl.BlockSpec((rows, bn), lambda i: (0, i)),
        out_shape=jax.ShapeDtypeStruct((rows, cols), BF),
        compiler_params=params(), name='q_proj',
        cost_estimate=cost(2 * rows * width * cols, 2 * width * (rows + cols)),
    )(n, w_q, cos_full, sin_full)


def attn_kernel(row0, chunk, bounds_ref, q_ref, k_ref, v_ref, ka, va, kb, vb, kc, vc, wo_ref, part_ref,
                wo_buf, k_buf, v_buf, o_buf, m_sc, l_sc, acc_sc, wo_sem, kv_sem):
    wo_copy = pltpu.make_async_copy(wo_ref, wo_buf, wo_sem)
    copies = []
    for slot, (ks, vs) in enumerate(((ka, va), (kb, vb), (kc, vc))):
        copies.append(pltpu.make_async_copy(ks, k_buf.at[slot], kv_sem.at[2 * slot]))
        copies.append(pltpu.make_async_copy(vs, v_buf.at[slot], kv_sem.at[2 * slot + 1]))
    for c in copies:
        c.start()
    wo_copy.start()
    n_kv = k_ref.shape[1] // HEAD_DIM
    groups = q_ref.shape[1] // k_ref.shape[1]
    stacked = groups * chunk
    n_keys = row0 + chunk
    for c in copies:
        c.wait()

    def head_step(g, carry):
        kcol = pl.ds(pl.multiple_of(g * HEAD_DIM, HEAD_DIM), HEAD_DIM)
        heads = [q_ref[:, pl.ds(pl.multiple_of((g * groups + j) * HEAD_DIM, HEAD_DIM), HEAD_DIM)] for j in range(groups)]
        q = jnp.concatenate(heads, axis=0)
        s = lax.dot_general(q, k_ref[:n_keys, kcol], (((1,), (1,)), ((), ())), preferred_element_type=F32)
        qpos = row0 + lax.rem(lax.broadcasted_iota(jnp.int32, (stacked, n_keys), 0), chunk)
        kpos = lax.broadcasted_iota(jnp.int32, (stacked, n_keys), 1)
        s = jnp.where(kpos <= qpos, s, MASK_VALUE)
        m0 = jnp.max(s, axis=-1, keepdims=True)
        p = jnp.exp2(s * EXP2_SCALE - m0 * EXP2_SCALE)
        m_sc[...] = jnp.broadcast_to(m0, m_sc.shape)
        l_sc[...] = jnp.broadcast_to(jnp.sum(p, axis=-1, keepdims=True), l_sc.shape)
        acc_sc[...] = jnp.dot(p.astype(BF), v_ref[:n_keys, kcol], preferred_element_type=F32)

        def block_step(b, carry2):
            s = lax.dot_general(q, k_buf[b, :, kcol], (((1,), (1,)), ((), ())), preferred_element_type=F32)
            m_old = m_sc[...]
            m_new = jnp.maximum(m_old, jnp.max(s, axis=-1, keepdims=True))
            alpha = jnp.exp2((m_old - m_new) * EXP2_SCALE)
            p = jnp.exp2(s * EXP2_SCALE - m_new[:, :1] * EXP2_SCALE)
            l_sc[...] = l_sc[...] * alpha + jnp.sum(p, axis=-1, keepdims=True)
            acc_sc[...] = acc_sc[...] * alpha + jnp.dot(p.astype(BF), v_buf[b, :, kcol], preferred_element_type=F32)
            m_sc[...] = m_new
            return carry2
        lax.fori_loop(bounds_ref[0], bounds_ref[1], block_step, 0)
        out = (acc_sc[...] / l_sc[...]).astype(BF)
        for j in range(groups):
            o_buf[:, pl.ds(pl.multiple_of((g * groups + j) * HEAD_DIM, HEAD_DIM), HEAD_DIM)] = out[j * chunk:(j + 1) * chunk]
        return carry
    lax.fori_loop(0, n_kv, head_step, 0)
    wo_copy.wait()

    def col_step(i, carry):
        cols = pl.ds(pl.multiple_of(i * 512, 512), 512)
        part_ref[:, cols] = jnp.dot(o_buf[...], wo_buf[:, cols], preferred_element_type=F32).astype(BF)
        return carry
    lax.fori_loop(0, part_ref.shape[1] // 512, col_step, 0)


def attn_chunk(row0, chunk, bounds, q, k, v, others, w_o):
    rows, qcols = q.shape
    kcols = k.shape[1]
    width = w_o.shape[1]
    stacked = chunk * (qcols // kcols)
    vmem = lambda a: pl.BlockSpec(a.shape, lambda i: (0, 0))
    return pl.pallas_call(
        functools.partial(attn_kernel, row0, chunk), grid=(1,),
        in_specs=[SMEM, pl.BlockSpec((chunk, qcols), lambda i: (row0 // chunk, 0)), vmem(k), vmem(v)] + [ANY] * 7,
        out_specs=pl.BlockSpec((chunk, width), lambda i: (0, 0)),
        out_shape=jax.ShapeDtypeStruct((chunk, width), BF),
        scratch_shapes=[pltpu.VMEM(w_o.shape, BF), pltpu.VMEM((3, rows, kcols), BF), pltpu.VMEM((3, rows, kcols), BF),
                        pltpu.VMEM((chunk, qcols), BF), pltpu.VMEM((stacked, HEAD_DIM), F32), pltpu.VMEM((stacked, HEAD_DIM), F32),
                        pltpu.VMEM((stacked, HEAD_DIM), F32), pltpu.SemaphoreType.DMA, pltpu.SemaphoreType.DMA((6,))],
        compiler_params=params(), name='attn_%d' % row0,
        cost_estimate=cost(2 * chunk * qcols * width + 8 * chunk * rows * qcols, 2 * qcols * width),
    )(bounds, q, k, v, *others, w_o)


def gate_up_kernel(n_parts, *refs):
    x_ref, gain_ref = refs[0], refs[1]
    parts = refs[2:2 + 2 * n_parts]
    wg_ref, wu_ref, h_ref, act_ref, m_buf = refs[2 + 2 * n_parts:]

    @pl.when(pl.program_id(0) == 0)
    def _():
        sub = x_ref.shape[0] // n_parts
        for i in range(n_parts):
            mine, other = parts[2 * i], parts[2 * i + 1]

            def chunk(j, c, i=i, mine=mine, other=other):
                src = pl.ds(pl.multiple_of(j * 32, 32), 32)
                dst = pl.ds(pl.multiple_of(i * sub + j * 32, 32), 32)
                total = mine[src, :].astype(F32) + other[src, :].astype(F32)
                h = (x_ref[dst, :].astype(F32) + total).astype(BF)
                h_ref[dst, :] = h
                m_buf[dst, :] = norm_rows(h.astype(F32), gain_ref[...])
                return c
            lax.fori_loop(0, sub // 32, chunk, 0)
    m = m_buf[...]
    gate = jnp.dot(m, wg_ref[...], preferred_element_type=F32)
    up = jnp.dot(m, wu_ref[...], preferred_element_type=F32)
    act_ref[...] = (gate / (1.0 + jnp.exp(-gate)) * up).astype(BF)


def gate_up(x, row0, rows, gain, parts, w_gate, w_up):
    width = x.shape[1]
    cols = w_gate.shape[1]
    bn = 512
    whole = lambda a: pl.BlockSpec(a.shape, lambda i: (0, 0))
    wspec = pl.BlockSpec((width, bn), lambda i: (0, i))
    n_parts = len(parts) // 2
    return pl.pallas_call(
        functools.partial(gate_up_kernel, n_parts), grid=(cols // bn,),
        in_specs=[pl.BlockSpec((rows, width), lambda i: (row0 // rows, 0)), whole(gain)] + [whole(p) for p in parts] + [wspec, wspec],
        out_specs=[pl.BlockSpec((rows, width), lambda i: (0, 0)), pl.BlockSpec((rows, bn), lambda i: (0, i))],
        out_shape=[jax.ShapeDtypeStruct((rows, width), BF), jax.ShapeDtypeStruct((rows, cols), BF)],
        scratch_shapes=[pltpu.VMEM((rows, width), BF)],
        compiler_params=params(), name='gate_up_%d' % row0,
        cost_estimate=cost(4 * rows * width * cols, 4 * width * cols),
    )(x, gain, *parts, w_gate, w_up)


def down_kernel(act_ref, w_ref, out_ref):
    out_ref[...] = jnp.dot(act_ref[...], w_ref[...], preferred_element_type=F32).astype(BF)


def down(act, w_down, col0, cols, tag):
    rows, depth = act.shape
    bn = 512
    return pl.pallas_call(
        down_kernel, grid=(cols // bn,),
        in_specs=[pl.BlockSpec((rows, depth), lambda i: (0, 0)), pl.BlockSpec((depth, bn), lambda i: (0, i + col0 // bn))],
        out_specs=pl.BlockSpec((rows, bn), lambda i: (0, i)),
        out_shape=jax.ShapeDtypeStruct((rows, cols), BF),
        compiler_params=params(), name='down_%s_%d' % (tag, col0),
        cost_estimate=cost(2 * rows * depth * cols, 2 * depth * cols),
    )(act, w_down)


def solution(mesh):
    row_spec = P(('dp', 'cp'), None)
    cache_spec = P(('dp', 'cp'), 'tp', None)
    col_spec = P(None, 'tp')
    split_rows = P('tp', None)
    vec_spec = P(None)
    swap = [(0, 1), (1, 0)]

    def local_layer(x, attn_gain, w_q, w_k, w_v, w_o, mlp_gain, w_gate, w_up, w_down):
        tok = x.shape[0]
        kv_local = w_k.shape[1] // HEAD_DIM
        cp_index = lax.axis_index('cp')
        cos_tab, sin_tab = rope_tables(cp_index * tok + jnp.arange(tok))
        cos_full = jnp.concatenate([cos_tab, cos_tab], axis=1)
        sin_full = jnp.concatenate([-sin_tab, sin_tab], axis=1)
        n, k, v = kv_proj(x, attn_gain[None, :], w_k, w_v, cos_full, sin_full)
        kb = lax.ppermute(k, 'cp', [(0, 2), (1, 3)])
        vb = lax.ppermute(v, 'cp', [(0, 2), (1, 3)])
        ka = lax.ppermute(k, 'cp', [(0, 1), (2, 3)])
        va = lax.ppermute(v, 'cp', [(0, 1), (2, 3)])
        kc = lax.ppermute(kb, 'cp', [(2, 3), (3, 2)])
        vc = lax.ppermute(vb, 'cp', [(2, 3), (3, 2)])
        q = q_proj(n, w_q, cos_full, sin_full)
        lo = jnp.where(cp_index == 2, 1, 0)
        hi = jnp.where(cp_index == 0, 0, jnp.where(cp_index == 1, 1, 3))
        bounds = jnp.stack([lo, hi]).astype(jnp.int32)
        others = (ka, va, kb, vb, kc, vc)
        chunk = 128
        mine, theirs = [], []
        for i in range(tok // chunk):
            part = attn_chunk(i * chunk, chunk, bounds, q, k, v, others, w_o)
            mine.append(part)
            theirs.append(lax.ppermute(part, 'tp', swap))
        half = tok // 2
        per = half // chunk
        outs = []
        pieces = (1024, 1024, 2048)
        for s in range(2):
            parts = []
            for i in range(s * per, (s + 1) * per):
                parts += [mine[i], theirs[i]]
            h, act = gate_up(x, s * half, half, mlp_gain[None, :], parts, w_gate, w_up)
            col = 0
            row_out = []
            for wdt in pieces:
                d = down(act, w_down, col, wdt, 'ab'[s])
                r = lax.ppermute(d, 'tp', swap)
                row_out.append((h[:, col:col + wdt].astype(F32) + (d.astype(F32) + r.astype(F32))).astype(BF))
                col += wdt
            outs.append(jnp.concatenate(row_out, axis=1))
        x_out = jnp.concatenate(outs, axis=0)
        return x_out, k.reshape(tok, kv_local, HEAD_DIM), v.reshape(tok, kv_local, HEAD_DIM)

    return jax.shard_map(local_layer, mesh=mesh,
                         in_specs=(row_spec, vec_spec, col_spec, col_spec, col_spec, split_rows, vec_spec, col_spec, col_spec, split_rows),
                         out_specs=(row_spec, cache_spec, cache_spec), check_vma=False)
```

```python
import functools
import jax
import jax.numpy as jnp
from jax import lax
from jax.experimental import pallas as pl
from jax.experimental.pallas import tpu as pltpu
from jax.sharding import PartitionSpec as P

HEAD_DIM = 128
ROPE_THETA = 1000000.0
NORM_EPS = 1e-5
MASK_VALUE = -1e30
EXP2_SCALE = HEAD_DIM ** -0.5 * 1.4426950408889634
BF = jnp.bfloat16
F32 = jnp.float32
VMEM_BIG = 60 * 1024 * 1024
ANY = pl.BlockSpec(memory_space=pl.ANY)


def cost(flops, nbytes):
    return pl.CostEstimate(flops=flops, bytes_accessed=nbytes, transcendentals=0)


def params():
    return pltpu.CompilerParams(vmem_limit_bytes=VMEM_BIG)


def rope_tables(positions):
    inv_freq = jnp.asarray(ROPE_THETA, F32) ** (-jnp.arange(0, HEAD_DIM, 2, dtype=F32) / HEAD_DIM)
    angles = positions.astype(F32)[:, None] * inv_freq[None, :]
    return jnp.cos(angles), jnp.sin(angles)


def norm_rows(rows, gain_row):
    inv_rms = lax.rsqrt(jnp.mean(rows * rows, axis=-1, keepdims=True) + NORM_EPS)
    return (rows * inv_rms * gain_row.astype(F32)).astype(BF)


def rope_block(prod, cos_full, sin_full):
    pieces = []
    for head in range(prod.shape[1] // HEAD_DIM):
        u = prod[:, head * HEAD_DIM:(head + 1) * HEAD_DIM].astype(BF).astype(F32)
        pieces.append((u * cos_full + pltpu.roll(u, HEAD_DIM // 2, 1) * sin_full).astype(BF))
    return jnp.concatenate(pieces, axis=1)


def kv_kernel(x_ref, gain_ref, wk_ref, wv_ref, cos_ref, sin_ref, n_ref, kv_ref):
    step = pl.program_id(0)

    @pl.when(step == 0)
    def _():
        def chunk(i, c):
            rows = pl.ds(pl.multiple_of(i * 64, 64), 64)
            n_ref[rows, :] = norm_rows(x_ref[rows, :].astype(F32), gain_ref[...])
            return c
        lax.fori_loop(0, x_ref.shape[0] // 64, chunk, 0)
    n = n_ref[...]
    bn = wk_ref.shape[1]
    cols = kv_ref.shape[1] // 2
    k = jnp.dot(n, wk_ref[...], preferred_element_type=F32)
    kv_ref[:, pl.ds(pl.multiple_of(step * bn, bn), bn)] = rope_block(k, cos_ref[...], sin_ref[...])
    kv_ref[:, pl.ds(pl.multiple_of(cols + step * bn, bn), bn)] = jnp.dot(n, wv_ref[...], preferred_element_type=F32).astype(BF)


def kv_proj(x, gain, w_k, w_v, cos_full, sin_full):
    rows, width = x.shape
    cols = w_k.shape[1]
    bn = 256
    whole = lambda a: pl.BlockSpec(a.shape, lambda i: (0, 0))
    wspec = pl.BlockSpec((width, bn), lambda i: (0, i))
    return pl.pallas_call(
        kv_kernel, grid=(cols // bn,),
        in_specs=[whole(x), whole(gain), wspec, wspec, whole(cos_full), whole(sin_full)],
        out_specs=[pl.BlockSpec((rows, width), lambda i: (0, 0)), pl.BlockSpec((rows, 2 * cols), lambda i: (0, 0))],
        out_shape=[jax.ShapeDtypeStruct((rows, width), BF), jax.ShapeDtypeStruct((rows, 2 * cols), BF)],
        compiler_params=params(), name='kv_proj',
        cost_estimate=cost(4 * rows * width * cols, 2 * 2 * width * (rows + cols)),
    )(x, gain, w_k, w_v, cos_full, sin_full)


def q_kernel(n_ref, w_ref, cos_ref, sin_ref, q_ref):
    prod = jnp.dot(n_ref[...], w_ref[...], preferred_element_type=F32)
    q_ref[...] = rope_block(prod, cos_ref[...], sin_ref[...])


def q_proj(n, w_q, cos_full, sin_full):
    rows, width = n.shape
    cols = w_q.shape[1]
    bn = 512
    whole = lambda a: pl.BlockSpec(a.shape, lambda i: (0, 0))
    return pl.pallas_call(
        q_kernel, grid=(cols // bn,),
        in_specs=[whole(n), pl.BlockSpec((width, bn), lambda i: (0, i)), whole(cos_full), whole(sin_full)],
        out_specs=pl.BlockSpec((rows, bn), lambda i: (0, i)),
        out_shape=jax.ShapeDtypeStruct((rows, cols), BF),
        compiler_params=params(), name='q_proj',
        cost_estimate=cost(2 * rows * width * cols, 2 * width * (rows + cols)),
    )(n, w_q, cos_full, sin_full)


MESH = pl.DeviceIdType.MESH
CHUNK = 128
HALF = 256
BLK = 512


def at(i, size):
    return pl.ds(pl.multiple_of(i * size, size), size)


def layer_kernel(gain_ref, q_ref, kv_ref, x_ref, kva, kvb, kvc, wo_ref, wg_ref, wu_ref, wd_ref, out_ref,
                 send_buf, recv_buf, h_buf, m_buf, act_buf, g_buf, u_buf, d_buf, k_buf, o_buf, m_sc, l_sc, acc_sc,
                 kv_sem, x_sem, wo_sem, g_sem, u_sem, d_sem, ps_sem, pr_sem, ds_sem, dr_sem, out_sem, free_sem):
    cp = lax.axis_index('cp')
    peer = {'tp': 1 - lax.axis_index('tp')}
    tok, width = q_ref.shape[0], wo_ref.shape[1]
    n_blk = width // BLK
    n_gu = wg_ref.shape[1] // BLK
    kcols = kv_ref.shape[1] // 2
    n_kv = kcols // HEAD_DIM
    groups = q_ref.shape[1] // kcols
    n_chunk = tok // CHUNK
    depth_o = wo_ref.shape[0]
    ring = 2 * (d_buf.shape[1] // depth_o)
    stacked = groups * CHUNK

    def load_wo(t):
        slot = lax.rem(t, ring)
        dst = d_buf.at[slot // (ring // 2), at(lax.rem(slot, ring // 2), depth_o), :]
        return pltpu.make_async_copy(wo_ref.at[:, at(lax.rem(t, n_blk), BLK)], dst, wo_sem.at[slot])

    def load_gate(t):
        cols = at(lax.rem(t, n_gu), BLK)
        slot = lax.rem(t, 2)
        return (pltpu.make_async_copy(wg_ref.at[:, cols], g_buf.at[slot], g_sem.at[slot]),
                pltpu.make_async_copy(wu_ref.at[:, cols], u_buf.at[slot], u_sem.at[slot]))

    def load_down(t):
        slot = lax.rem(t, 2)
        return pltpu.make_async_copy(wd_ref.at[:, at(lax.rem(t, n_blk), BLK)], d_buf.at[slot], d_sem.at[slot])

    def load_x(j):
        return pltpu.make_async_copy(x_ref.at[:, at(j, BLK)], h_buf.at[j], x_sem.at[j])

    def part_copy(i, j):
        piece = (j, at(i, CHUNK), slice(None))
        return pltpu.make_async_remote_copy(send_buf.at[piece], recv_buf.at[piece], ps_sem.at[i, j], pr_sem.at[i, j],
                                            device_id=peer, device_id_type=MESH)

    def down_copy(s, j):
        piece = (j, at(s, HALF), slice(None))
        return pltpu.make_async_remote_copy(send_buf.at[piece], recv_buf.at[piece], ds_sem.at[s, j], dr_sem.at[s, j],
                                            device_id=peer, device_id_type=MESH)

    def out_copy(s, j):
        return pltpu.make_async_copy(h_buf.at[j, at(s, HALF), :], out_ref.at[at(s, HALF), at(j, BLK)], out_sem.at[s, j])

    def loop(n, body):
        def step(i, c):
            body(i)
            return c
        lax.fori_loop(0, n, step, 0)

    kv_copies = [pltpu.make_async_copy(src, k_buf.at[slot], kv_sem.at[slot]) for slot, src in enumerate((kva, kvb, kvc))]
    for c in kv_copies:
        c.start()
    loop(ring - 1, lambda t: load_wo(t).start())
    loop(n_blk, lambda j: load_x(j).start())
    for c in load_gate(0):
        c.start()

    barrier = pltpu.get_barrier_semaphore()
    pl.semaphore_signal(barrier, inc=1, device_id=peer, device_id_type=MESH)
    pl.semaphore_wait(barrier, 1)

    for c in kv_copies:
        c.wait()
    lo = jnp.where(cp == 2, 1, 0)
    hi = jnp.where(cp == 0, 0, jnp.where(cp == 1, 1, 3))

    for i in range(n_chunk):
        row0 = i * CHUNK
        n_keys = row0 + CHUNK

        def head_step(g):
            kcol = at(g, HEAD_DIM)
            vcol = pl.ds(pl.multiple_of(kcols + g * HEAD_DIM, HEAD_DIM), HEAD_DIM)
            q = jnp.concatenate([q_ref[row0:row0 + CHUNK, at(g * groups + j, HEAD_DIM)] for j in range(groups)], axis=0)
            s = lax.dot_general(q, kv_ref[:n_keys, kcol], (((1,), (1,)), ((), ())), preferred_element_type=F32)
            qpos = row0 + lax.rem(lax.broadcasted_iota(jnp.int32, (stacked, n_keys), 0), CHUNK)
            kpos = lax.broadcasted_iota(jnp.int32, (stacked, n_keys), 1)
            s = jnp.where(kpos <= qpos, s, MASK_VALUE)
            m0 = jnp.max(s, axis=-1, keepdims=True)
            p = jnp.exp2(s * EXP2_SCALE - m0 * EXP2_SCALE)
            m_sc[...] = jnp.broadcast_to(m0, m_sc.shape)
            l_sc[...] = jnp.broadcast_to(jnp.sum(p, axis=-1, keepdims=True), l_sc.shape)
            acc_sc[...] = jnp.dot(p.astype(BF), kv_ref[:n_keys, vcol], preferred_element_type=F32)

            def block_step(b, c):
                s = lax.dot_general(q, k_buf[b, :, kcol], (((1,), (1,)), ((), ())), preferred_element_type=F32)
                m_old = m_sc[...]
                m_new = jnp.maximum(m_old, jnp.max(s, axis=-1, keepdims=True))
                alpha = jnp.exp2((m_old - m_new) * EXP2_SCALE)
                p = jnp.exp2(s * EXP2_SCALE - m_new[:, :1] * EXP2_SCALE)
                l_sc[...] = l_sc[...] * alpha + jnp.sum(p, axis=-1, keepdims=True)
                acc_sc[...] = acc_sc[...] * alpha + jnp.dot(p.astype(BF), k_buf[b, :, vcol], preferred_element_type=F32)
                m_sc[...] = m_new
                return c
            lax.fori_loop(lo, hi, block_step, 0)
            out = (acc_sc[...] / l_sc[...]).astype(BF)
            for j in range(groups):
                o_buf[:, at(g * groups + j, HEAD_DIM)] = out[j * CHUNK:(j + 1) * CHUNK]
        loop(n_kv, head_step)

        def wo_step(j):
            t = i * n_blk + j

            @pl.when(t + ring - 1 < n_chunk * n_blk)
            def _():
                load_wo(t + ring - 1).start()
            load_wo(t).wait()
            slot = lax.rem(t, ring)
            w = d_buf[slot // (ring // 2), at(lax.rem(slot, ring // 2), depth_o), :]
            send_buf[j, row0:row0 + CHUNK, :] = jnp.dot(o_buf[...], w, preferred_element_type=F32).astype(BF)
            part_copy(i, j).start()
        loop(n_blk, wo_step)

    loop(n_blk, lambda j: load_x(j).wait())

    def half_step(s):
        def wait_part(r):
            c = part_copy(s * (HALF // CHUNK) + r // n_blk, lax.rem(r, n_blk))
            c.wait_recv()
            c.wait_send()
        loop(HALF // CHUNK * n_blk, wait_part)

        def h_step(r):
            rows = at(s * (HALF // 32) + r, 32)
            total = jnp.zeros((32, BLK), F32)
            for j in range(n_blk):
                add = send_buf[j, rows, :].astype(F32) + recv_buf[j, rows, :].astype(F32)
                h = (h_buf[j, rows, :].astype(F32) + add).astype(BF)
                h_buf[j, rows, :] = h
                wide = h.astype(F32)
                total += wide * wide
            inv = lax.rsqrt(jnp.sum(total, axis=-1, keepdims=True) / width + NORM_EPS)
            for j in range(n_blk):
                cols = slice(j * BLK, (j + 1) * BLK)
                m_buf[at(r, 32), cols] = (h_buf[j, rows, :].astype(F32) * inv * gain_ref[:, cols].astype(F32)).astype(BF)
        loop(HALF // 32, h_step)
        pl.semaphore_signal(free_sem.at[s], inc=1, device_id=peer, device_id_type=MESH)

        def gu_step(j):
            t = s * n_gu + j

            @pl.when(t + 1 < 2 * n_gu)
            def _():
                for c in load_gate(t + 1):
                    c.start()

            @pl.when(j == n_gu - 4)
            def _():
                load_down(s * n_blk).start()

            @pl.when(j == n_gu - 2)
            def _():
                load_down(s * n_blk + 1).start()
            for c in load_gate(t):
                c.wait()
            slot = lax.rem(t, 2)
            gate = jnp.dot(m_buf[...], g_buf[slot], preferred_element_type=F32)
            up = jnp.dot(m_buf[...], u_buf[slot], preferred_element_type=F32)
            act_buf[:, at(j, BLK)] = (gate / (1.0 + jnp.exp(-gate)) * up).astype(BF)
        loop(n_gu, gu_step)
        pl.semaphore_wait(free_sem.at[s], 1)

        def down_step(j):
            t = s * n_blk + j
            load_down(t).wait()
            send_buf[j, at(s, HALF), :] = jnp.dot(act_buf[...], d_buf[lax.rem(t, 2)], preferred_element_type=F32).astype(BF)

            @pl.when(j + 2 < n_blk)
            def _():
                load_down(t + 2).start()
            down_copy(s, j).start()
        loop(n_blk, down_step)
    loop(2, half_step)

    def final_step(t):
        s, j = t // n_blk, lax.rem(t, n_blk)
        c = down_copy(s, j)
        c.wait_recv()
        rows = at(s, HALF)
        add = send_buf[j, rows, :].astype(F32) + recv_buf[j, rows, :].astype(F32)
        h_buf[j, rows, :] = (h_buf[j, rows, :].astype(F32) + add).astype(BF)
        out_copy(s, j).start()
    loop(2 * n_blk, final_step)

    def drain(t):
        s, j = t // n_blk, lax.rem(t, n_blk)
        down_copy(s, j).wait_send()
        out_copy(s, j).wait()
    loop(2 * n_blk, drain)


def fused_layer(gain, q, kv, x, kva, kvb, kvc, w_o, w_gate, w_up, w_down):
    tok, width = x.shape
    qcols = q.shape[1]
    n_blk = width // BLK
    ff = w_gate.shape[1]
    n_chunk = tok // CHUNK
    stacked = CHUNK * (2 * qcols // kv.shape[1])
    vmem = pl.BlockSpec(memory_space=pltpu.VMEM)
    ring = 2 * (ff // qcols)
    dma = pltpu.SemaphoreType.DMA
    return pl.pallas_call(
        layer_kernel,
        in_specs=[vmem, vmem, vmem] + [ANY] * 8,
        out_specs=ANY,
        out_shape=jax.ShapeDtypeStruct((tok, width), BF),
        scratch_shapes=[
            pltpu.VMEM((n_blk, tok, BLK), BF), pltpu.VMEM((n_blk, tok, BLK), BF), pltpu.VMEM((n_blk, tok, BLK), BF),
            pltpu.VMEM((HALF, width), BF), pltpu.VMEM((HALF, ff), BF),
            pltpu.VMEM((2, width, BLK), BF), pltpu.VMEM((2, width, BLK), BF), pltpu.VMEM((2, ff, BLK), BF),
            pltpu.VMEM((3,) + kv.shape, BF), pltpu.VMEM((CHUNK, qcols), BF),
            pltpu.VMEM((stacked, HEAD_DIM), F32), pltpu.VMEM((stacked, HEAD_DIM), F32), pltpu.VMEM((stacked, HEAD_DIM), F32),
            dma((3,)), dma((n_blk,)), dma((ring,)), dma((2,)), dma((2,)), dma((2,)),
            dma((n_chunk, n_blk)), dma((n_chunk, n_blk)), dma((2, n_blk)), dma((2, n_blk)), dma((2, n_blk)),
            pltpu.SemaphoreType.REGULAR((2,))],
        compiler_params=pltpu.CompilerParams(vmem_limit_bytes=67043328, collective_id=0, has_side_effects=True),
        name='fused_layer',
        cost_estimate=cost(2 * tok * width * (qcols + 3 * ff), 2 * width * (qcols + 6 * ff)),
    )(gain, q, kv, x, kva, kvb, kvc, w_o, w_gate, w_up, w_down)


def solution(mesh):
    row_spec = P(('dp', 'cp'), None)
    cache_spec = P(('dp', 'cp'), 'tp', None)
    col_spec = P(None, 'tp')
    split_rows = P('tp', None)
    vec_spec = P(None)

    def local_layer(x, attn_gain, w_q, w_k, w_v, w_o, mlp_gain, w_gate, w_up, w_down):
        tok = x.shape[0]
        kv_local = w_k.shape[1] // HEAD_DIM
        cp_index = lax.axis_index('cp')
        cos_tab, sin_tab = rope_tables(cp_index * tok + jnp.arange(tok))
        cos_full = jnp.concatenate([cos_tab, cos_tab], axis=1)
        sin_full = jnp.concatenate([-sin_tab, sin_tab], axis=1)
        n, kv = kv_proj(x, attn_gain[None, :], w_k, w_v, cos_full, sin_full)
        kvb = lax.ppermute(kv, 'cp', [(0, 2), (1, 3)])
        kva = lax.ppermute(kv, 'cp', [(0, 1), (2, 3)])
        q = q_proj(n, w_q, cos_full, sin_full)
        kvc = lax.ppermute(kvb, 'cp', [(2, 3), (3, 2)])
        x_out = fused_layer(mlp_gain[None, :], q, kv, x, kva, kvb, kvc, w_o, w_gate, w_up, w_down)
        kcols = kv.shape[1] // 2
        k, v = kv[:, :kcols], kv[:, kcols:]
        return x_out, k.reshape(tok, kv_local, HEAD_DIM), v.reshape(tok, kv_local, HEAD_DIM)

    return jax.shard_map(local_layer, mesh=mesh,
                         in_specs=(row_spec, vec_spec, col_spec, col_spec, col_spec, split_rows, vec_spec, col_spec, col_spec, split_rows),
                         out_specs=(row_spec, cache_spec, cache_spec), check_vma=False)
```

```python
import jax
import jax.numpy as jnp
from jax import lax
from jax.experimental import pallas as pl
from jax.experimental.pallas import tpu as pltpu
from jax.sharding import PartitionSpec as P

HEAD_DIM = 128
ROPE_THETA = 1000000.0
NORM_EPS = 1e-5
MASK_VALUE = -1e30
EXP2_SCALE = HEAD_DIM ** -0.5 * 1.4426950408889634
BF = jnp.bfloat16
F32 = jnp.float32
ANY = pl.BlockSpec(memory_space=pl.ANY)
VMEM = pl.BlockSpec(memory_space=pltpu.VMEM)
MESH = pl.DeviceIdType.MESH
LANES = 128
CHUNK = 128
HALF = 256
BLK = 512
SLOT = 2048
N_SLOT = 12


def at(i, size):
    return pl.ds(pl.multiple_of(i * size, size), size)


def loop(n, body):
    def step(i, c):
        body(i)
        return c
    lax.fori_loop(0, n, step, 0)


def rope_tables(positions):
    inv_freq = jnp.asarray(ROPE_THETA, F32) ** (-jnp.arange(0, HEAD_DIM, 2, dtype=F32) / HEAD_DIM)
    angles = positions.astype(F32)[:, None] * inv_freq[None, :]
    return jnp.cos(angles), jnp.sin(angles)


def layer_kernel(cos_ref, sin_ref, again_ref, mgain_ref, x_ref, wq_ref, wk_ref, wv_ref, wo_ref, wg_ref, wu_ref, wd_ref,
                 out_ref, kv_out_ref,
                 ring, send_buf, recv_buf, h_buf, n_buf, act_buf, kv_buf, q_buf, o_buf, m_sc, l_sc, acc_sc,
                 x_sem, wkv_sem, w_sem, kvs_sem, kvr_sem, kvo_sem, ps_sem, pr_sem, ds_sem, dr_sem, out_sem, free_sem):
    cp = lax.axis_index('cp')
    peer = {'tp': 1 - lax.axis_index('tp')}
    pair = {'cp': cp + 1 - 2 * lax.rem(cp, 2)}
    across = {'cp': lax.rem(cp + 2, 4)}
    tok, width = n_buf.shape
    n_blk = width // BLK
    n_gu = wg_ref.shape[1] // BLK
    n_q = wq_ref.shape[1] // BLK
    n_kv = wk_ref.shape[1] // HEAD_DIM
    groups = wq_ref.shape[1] // wk_ref.shape[1]
    n_chunk = tok // CHUNK
    stacked = groups * CHUNK
    gu_slots, d_slots = width // SLOT, wd_ref.shape[0] // SLOT
    gu_deep, d_deep = N_SLOT // (2 * gu_slots), N_SLOT // d_slots
    kv_slots = n_kv // 2 * gu_slots

    def ring_rows(slot, n):
        return pl.ds(pl.multiple_of(slot * SLOT, SLOT), n * SLOT)

    def load(src, slot, n):
        return pltpu.make_async_copy(src, ring.at[ring_rows(slot, n), :], w_sem.at[slot])

    def load_q(u):
        return load(wq_ref.at[:, at(u, BLK)], kv_slots + gu_slots * u, gu_slots)

    def load_wo(t):
        return load(wo_ref.at[:, at(lax.rem(t, n_blk), BLK)], lax.rem(t, N_SLOT), 1)

    def gate_slot(j):
        return lax.rem(j, gu_deep) * 2 * gu_slots

    def load_gate(j):
        return load(wg_ref.at[:, at(j, BLK)], gate_slot(j), gu_slots)

    def load_up(j):
        return load(wu_ref.at[:, at(j, BLK)], gate_slot(j) + gu_slots, gu_slots)

    def load_down(j):
        return load(wd_ref.at[:, at(j, BLK)], lax.rem(j, d_deep) * d_slots, d_slots)

    def load_kv(g, which):
        src = (wk_ref, wv_ref)[which]
        rows = pl.ds(g // 2 * gu_slots * SLOT, width)
        cols = pl.ds((g % 2) * 2 * HEAD_DIM + which * HEAD_DIM, HEAD_DIM)
        return pltpu.make_async_copy(src.at[:, pl.ds(g * HEAD_DIM, HEAD_DIM)], ring.at[rows, cols], wkv_sem.at[g, which])

    def load_x(j):
        return pltpu.make_async_copy(x_ref.at[:, at(j, BLK)], h_buf.at[j], x_sem.at[j])

    def kv_copy(kind, g):
        src_block = 2 if kind == 2 else 0
        return pltpu.make_async_remote_copy(kv_buf.at[src_block, g], kv_buf.at[kind + 1, g], kvs_sem.at[kind, g], kvr_sem.at[kind, g],
                                            device_id=across if kind == 1 else pair, device_id_type=MESH)

    def kv_out(g):
        return pltpu.make_async_copy(kv_buf.at[0, g], kv_out_ref.at[g], kvo_sem.at[g])

    def part_copy(i, j):
        piece = (j, at(i, CHUNK), slice(None))
        return pltpu.make_async_remote_copy(send_buf.at[piece], recv_buf.at[piece], ps_sem.at[i, j], pr_sem.at[i, j],
                                            device_id=peer, device_id_type=MESH)

    def down_copy(s, j):
        piece = (j, at(s, HALF), slice(None))
        return pltpu.make_async_remote_copy(send_buf.at[piece], recv_buf.at[piece], ds_sem.at[s, j], dr_sem.at[s, j],
                                            device_id=peer, device_id_type=MESH)

    def out_copy(s, j):
        return pltpu.make_async_copy(h_buf.at[j, at(s, HALF), :], out_ref.at[at(s, HALF), at(j, BLK)], out_sem.at[s, j])

    def scale_rows(src_rows, dst_rows, total, gain_ref):
        inv = lax.rsqrt(jnp.sum(total, axis=-1, keepdims=True) / width + NORM_EPS)
        for r in range(width // LANES):
            j, c = r * LANES // BLK, r * LANES % BLK
            wide = h_buf[j, src_rows, c:c + LANES].astype(F32)
            n_buf[dst_rows, r * LANES:(r + 1) * LANES] = (wide * inv * gain_ref[r:r + 1, :].astype(F32)).astype(BF)

    def rope(prod):
        cos_full = jnp.concatenate([cos_ref[...], cos_ref[...]], axis=1)
        sin_full = jnp.concatenate([-sin_ref[...], sin_ref[...]], axis=1)
        u = prod.astype(BF).astype(F32)
        return (u * cos_full + pltpu.roll(u, HEAD_DIM // 2, 1) * sin_full).astype(BF)

    loop(n_blk, lambda j: load_x(j).start())
    for g in range(n_kv):
        for which in range(2):
            load_kv(g, which).start()
    for u in range(n_q):
        load_q(u).start()
    barrier = pltpu.get_barrier_semaphore()
    for other in (peer, pair, across):
        pl.semaphore_signal(barrier, inc=1, device_id=other, device_id_type=MESH)
    loop(n_blk, lambda j: load_x(j).wait())

    def norm_step(r):
        rows = at(r, 32)
        total = jnp.zeros((32, BLK), F32)
        for j in range(n_blk):
            wide = h_buf[j, rows, :].astype(F32)
            total += wide * wide
        scale_rows(rows, rows, total, again_ref)
    loop(tok // 32, norm_step)

    for g in range(n_kv):
        for which in range(2):
            load_kv(g, which).wait()
        w = ring[g // 2 * gu_slots * SLOT:g // 2 * gu_slots * SLOT + width, (g % 2) * 2 * HEAD_DIM:(g % 2 + 1) * 2 * HEAD_DIM]
        prod = jnp.dot(n_buf[...], w, preferred_element_type=F32)
        kv_buf[0, g, :, :HEAD_DIM] = rope(prod[:, :HEAD_DIM])
        kv_buf[0, g, :, HEAD_DIM:] = prod[:, HEAD_DIM:].astype(BF)
        if g == 0:
            pl.semaphore_wait(barrier, 3)

        @pl.when(cp < 2)
        def _():
            kv_copy(1, g).start()

        @pl.when(lax.rem(cp, 2) == 0)
        def _():
            kv_copy(0, g).start()
        kv_out(g).start()
    for t in range(kv_slots):
        load_wo(t).start()

    def q_step(u):
        load_q(u).wait()
        w = ring[ring_rows(kv_slots + gu_slots * u, gu_slots), :]
        prod = jnp.dot(n_buf[...], w, preferred_element_type=F32)
        for j in range(BLK // HEAD_DIM):
            q_buf[:, pl.ds(pl.multiple_of(u * BLK + j * HEAD_DIM, HEAD_DIM), HEAD_DIM)] = rope(prod[:, j * HEAD_DIM:(j + 1) * HEAD_DIM])
        for t in range(gu_slots):
            load_wo(kv_slots + gu_slots * u + t).start()
    loop(n_q, q_step)

    lo = jnp.where(cp == 2, 2, 1)
    hi = jnp.where(cp == 0, 1, jnp.where(cp == 1, 2, 4))
    for i in range(n_chunk):
        row0 = i * CHUNK
        n_keys = row0 + CHUNK

        def head_step(g):
            q = jnp.concatenate([q_buf[row0:row0 + CHUNK, at(g * groups + j, HEAD_DIM)] for j in range(groups)], axis=0)
            s = lax.dot_general(q, kv_buf[0, g, :n_keys, :HEAD_DIM], (((1,), (1,)), ((), ())), preferred_element_type=F32)
            qpos = row0 + lax.rem(lax.broadcasted_iota(jnp.int32, (stacked, n_keys), 0), CHUNK)
            kpos = lax.broadcasted_iota(jnp.int32, (stacked, n_keys), 1)
            s = jnp.where(kpos <= qpos, s, MASK_VALUE)
            m0 = jnp.max(s, axis=-1, keepdims=True)
            p = jnp.exp2(s * EXP2_SCALE - m0 * EXP2_SCALE)
            m_sc[...] = jnp.broadcast_to(m0, m_sc.shape)
            l_sc[...] = jnp.broadcast_to(jnp.sum(p, axis=-1, keepdims=True), l_sc.shape)
            acc_sc[...] = jnp.dot(p.astype(BF), kv_buf[0, g, :n_keys, HEAD_DIM:], preferred_element_type=F32)

            def block_step(b, c):
                if i == 0:
                    @pl.when(b == 1)
                    def _():
                        kv_copy(0, g).wait_recv()

                    @pl.when(b == 2)
                    def _():
                        kv_copy(1, g).wait_recv()
                        kv_copy(2, g).start()

                    @pl.when(b == 3)
                    def _():
                        kv_copy(2, g).wait_recv()
                s = lax.dot_general(q, kv_buf[b, g, :, :HEAD_DIM], (((1,), (1,)), ((), ())), preferred_element_type=F32)
                m_old = m_sc[...]
                m_new = jnp.maximum(m_old, jnp.max(s, axis=-1, keepdims=True))
                alpha = jnp.exp2((m_old - m_new) * EXP2_SCALE)
                p = jnp.exp2(s * EXP2_SCALE - m_new[:, :1] * EXP2_SCALE)
                l_sc[...] = l_sc[...] * alpha + jnp.sum(p, axis=-1, keepdims=True)
                acc_sc[...] = acc_sc[...] * alpha + jnp.dot(p.astype(BF), kv_buf[b, g, :, HEAD_DIM:], preferred_element_type=F32)
                m_sc[...] = m_new
                return c
            lax.fori_loop(lo, hi, block_step, 0)
            out = (acc_sc[...] / l_sc[...]).astype(BF)
            for j in range(groups):
                o_buf[:, at(g * groups + j, HEAD_DIM)] = out[j * CHUNK:(j + 1) * CHUNK]
        loop(n_kv, head_step)

        def wo_step(j):
            t = i * n_blk + j
            load_wo(t).wait()
            w = ring[ring_rows(lax.rem(t, N_SLOT), 1), :]
            send_buf[j, row0:row0 + CHUNK, :] = jnp.dot(o_buf[...], w, preferred_element_type=F32).astype(BF)
            part_copy(i, j).start()
            if (i + 1) * n_blk - 1 + N_SLOT < n_chunk * n_blk:
                load_wo(t + N_SLOT).start()
            else:
                @pl.when(t + N_SLOT < n_chunk * n_blk)
                def _():
                    load_wo(t + N_SLOT).start()

                first = n_chunk * n_blk - N_SLOT
                for b in range(gu_deep):
                    end = 2 * gu_slots * b
                    for which in range(2):
                        last_slot = end + which * gu_slots + gu_slots - 1
                        when = first + (last_slot - first) % N_SLOT

                        @pl.when(t == when)
                        def _():
                            (load_gate, load_up)[which](b).start()
        loop(n_blk, wo_step)

    def half_step(s):
        def wait_part(r):
            c = part_copy(s * (HALF // CHUNK) + r // n_blk, lax.rem(r, n_blk))
            c.wait_recv()
            c.wait_send()
        loop(HALF // CHUNK * n_blk, wait_part)

        def h_step(r):
            rows = at(s * (HALF // 32) + r, 32)
            total = jnp.zeros((32, BLK), F32)
            for j in range(n_blk):
                add = send_buf[j, rows, :].astype(F32) + recv_buf[j, rows, :].astype(F32)
                h = (h_buf[j, rows, :].astype(F32) + add).astype(BF)
                h_buf[j, rows, :] = h
                wide = h.astype(F32)
                total += wide * wide
            scale_rows(rows, at(r, 32), total, mgain_ref)
        loop(HALF // 32, h_step)
        pl.semaphore_signal(free_sem.at[s], inc=1, device_id=peer, device_id_type=MESH)

        def gu_step(j):
            slot = gate_slot(j)
            load_gate(j).wait()
            gate = jnp.dot(n_buf[:HALF, :], ring[ring_rows(slot, gu_slots), :], preferred_element_type=F32)
            load_up(j).wait()
            up = jnp.dot(n_buf[:HALF, :], ring[ring_rows(slot + gu_slots, gu_slots), :], preferred_element_type=F32)
            act_buf[:, at(j, BLK)] = (gate / (1.0 + jnp.exp(-gate)) * up).astype(BF)

            @pl.when(j + gu_deep < n_gu)
            def _():
                load_gate(j + gu_deep).start()
                load_up(j + gu_deep).start()
            freed = 0
            for back in range(gu_deep, 0, -1):
                now = (2 * gu_slots * (gu_deep - back + 1)) // d_slots

                @pl.when(j == n_gu - back)
                def _():
                    for d in range(freed, now):
                        load_down(d).start()
                freed = now
        loop(n_gu, gu_step)
        pl.semaphore_wait(free_sem.at[s], 1)

        def down_step(j):
            load_down(j).wait()
            w = ring[ring_rows(lax.rem(j, d_deep) * d_slots, d_slots), :]
            send_buf[j, at(s, HALF), :] = jnp.dot(act_buf[...], w, preferred_element_type=F32).astype(BF)
            down_copy(s, j).start()

            @pl.when(j + d_deep < n_blk)
            def _():
                load_down(j + d_deep).start()
            freed = 0
            for back in range(d_deep, 0, -1):
                now = d_slots * (d_deep - back + 1) // gu_slots

                @pl.when((j == n_blk - back) & (s == 0))
                def _():
                    for d in range(freed, now):
                        (load_gate, load_up)[d % 2](d // 2).start()
                freed = now
        loop(n_blk, down_step)
    loop(tok // HALF, half_step)

    def final_step(t):
        s, j = t // n_blk, lax.rem(t, n_blk)
        down_copy(s, j).wait_recv()
        rows = at(s, HALF)
        add = send_buf[j, rows, :].astype(F32) + recv_buf[j, rows, :].astype(F32)
        h_buf[j, rows, :] = (h_buf[j, rows, :].astype(F32) + add).astype(BF)
        out_copy(s, j).start()
    loop(tok // HALF * n_blk, final_step)

    def drain(t):
        s, j = t // n_blk, lax.rem(t, n_blk)
        down_copy(s, j).wait_send()
        out_copy(s, j).wait()
    loop(tok // HALF * n_blk, drain)
    for g in range(n_kv):
        kv_out(g).wait()

        @pl.when(cp < 2)
        def _():
            kv_copy(1, g).wait_send()

        @pl.when(lax.rem(cp, 2) == 0)
        def _():
            kv_copy(0, g).wait_send()

        @pl.when(cp >= 2)
        def _():
            kv_copy(2, g).wait_send()


def fused_layer(cos_tab, sin_tab, attn_gain, mlp_gain, x, w_q, w_k, w_v, w_o, w_gate, w_up, w_down):
    tok, width = x.shape
    qcols, kcols, ff = w_q.shape[1], w_k.shape[1], w_gate.shape[1]
    n_blk, n_chunk, n_kv, halves = width // BLK, tok // CHUNK, kcols // HEAD_DIM, tok // HALF
    stacked = CHUNK * (qcols // kcols)
    dma = pltpu.SemaphoreType.DMA
    return pl.pallas_call(
        layer_kernel,
        in_specs=[VMEM] * 4 + [ANY] * 8,
        out_specs=[ANY, ANY],
        out_shape=[jax.ShapeDtypeStruct((tok, width), BF), jax.ShapeDtypeStruct((n_kv, tok, 2 * HEAD_DIM), BF)],
        scratch_shapes=[
            pltpu.VMEM((N_SLOT * SLOT, BLK), BF),
            pltpu.VMEM((n_blk, tok, BLK), BF), pltpu.VMEM((n_blk, tok, BLK), BF), pltpu.VMEM((n_blk, tok, BLK), BF),
            pltpu.VMEM((tok, width), BF), pltpu.VMEM((HALF, ff), BF),
            pltpu.VMEM((4, n_kv, tok, 2 * HEAD_DIM), BF), pltpu.VMEM((tok, qcols), BF), pltpu.VMEM((CHUNK, qcols), BF),
            pltpu.VMEM((stacked, HEAD_DIM), F32), pltpu.VMEM((stacked, HEAD_DIM), F32), pltpu.VMEM((stacked, HEAD_DIM), F32),
            dma((n_blk,)), dma((n_kv, 2)), dma((N_SLOT,)), dma((3, n_kv)), dma((3, n_kv)), dma((n_kv,)),
            dma((n_chunk, n_blk)), dma((n_chunk, n_blk)), dma((halves, n_blk)), dma((halves, n_blk)), dma((halves, n_blk)),
            pltpu.SemaphoreType.REGULAR((halves,))],
        compiler_params=pltpu.CompilerParams(vmem_limit_bytes=67043328, collective_id=0, has_side_effects=True),
        name='fused_layer',
        cost_estimate=pl.CostEstimate(flops=2 * tok * width * (2 * qcols + 2 * kcols + 3 * ff), transcendentals=0,
                                      bytes_accessed=2 * width * (2 * qcols + 2 * kcols + 6 * ff)),
    )(cos_tab, sin_tab, attn_gain, mlp_gain, x, w_q, w_k, w_v, w_o, w_gate, w_up, w_down)


def emit_kernel(y_ref, kv_ref, x_out_ref, k_ref, v_ref):
    x_out_ref[...] = y_ref[...]
    for g in range(kv_ref.shape[0]):
        k_ref[:, g, :] = kv_ref[g, :, :HEAD_DIM]
        v_ref[:, g, :] = kv_ref[g, :, HEAD_DIM:]


def emit(y, kv):
    tok, width = y.shape
    n_kv = kv.shape[0]
    rows = 128
    cache = pl.BlockSpec((rows, n_kv, HEAD_DIM), lambda i: (i, 0, 0))
    return pl.pallas_call(
        emit_kernel, grid=(tok // rows,),
        in_specs=[pl.BlockSpec((rows, width), lambda i: (i, 0)), pl.BlockSpec((n_kv, rows, 2 * HEAD_DIM), lambda i: (0, i, 0))],
        out_specs=[pl.BlockSpec((rows, width), lambda i: (i, 0)), cache, cache],
        out_shape=[jax.ShapeDtypeStruct((tok, width), BF)] + [jax.ShapeDtypeStruct((tok, n_kv, HEAD_DIM), BF)] * 2,
        name='emit',
    )(y, kv)


def solution(mesh):
    row_spec = P(('dp', 'cp'), None)
    cache_spec = P(('dp', 'cp'), 'tp', None)
    col_spec = P(None, 'tp')
    split_rows = P('tp', None)
    vec_spec = P(None)

    def local_layer(x, attn_gain, w_q, w_k, w_v, w_o, mlp_gain, w_gate, w_up, w_down):
        tok, width = x.shape
        cos_tab, sin_tab = rope_tables(lax.axis_index('cp') * tok + jnp.arange(tok))
        gains = [g.reshape(width // LANES, LANES) for g in (attn_gain, mlp_gain)]
        y, kv = fused_layer(cos_tab, sin_tab, *gains, x, w_q, w_k, w_v, w_o, w_gate, w_up, w_down)
        return tuple(emit(y, kv))

    return jax.shard_map(local_layer, mesh=mesh,
                         in_specs=(row_spec, vec_spec, col_spec, col_spec, col_spec, split_rows, vec_spec, col_spec, col_spec, split_rows),
                         out_specs=(row_spec, cache_spec, cache_spec), check_vma=False)
```

```python
import jax
import jax.numpy as jnp
import numpy as np
from jax import lax
from jax.experimental import pallas as pl
from jax.experimental.pallas import tpu as pltpu
from jax.sharding import PartitionSpec as P

HEAD_DIM = 128
ROPE_THETA = 1000000.0
NORM_EPS = 1e-5
MASK_VALUE = -1e30
EXP2_SCALE = HEAD_DIM ** -0.5 * 1.4426950408889634
BF = jnp.bfloat16
F32 = jnp.float32
ANY = pl.BlockSpec(memory_space=pl.ANY)
VMEM = pl.BlockSpec(memory_space=pltpu.VMEM)
MESH = pl.DeviceIdType.MESH
LANES = 128
CHUNK = 128
HALF = 256
BLK = 512
SLOT = 2048
X_ROWS = 64
KV_ROWS = 128
N_SLOT = 12
VMEM_LIMIT = 60000000


def at(i, size):
    return pl.ds(pl.multiple_of(i * size, size), size)


def loop(n, body):
    def step(i, c):
        body(i)
        return c
    lax.fori_loop(0, n, step, 0)


def rope_table(n_pos):
    inv_freq = np.float32(ROPE_THETA) ** (-np.arange(0, HEAD_DIM, 2, dtype=np.float32) / np.float32(HEAD_DIM))
    angles = np.arange(n_pos, dtype=np.float32)[:, None] * inv_freq[None, :]
    return np.concatenate([np.cos(angles), np.sin(angles)], axis=1).astype(np.float32)


def layer_kernel(tab_ref, again_ref, mgain_ref, x_ref, wq_ref, wk_ref, wv_ref, wo_ref, wg_ref, wu_ref, wd_ref,
                 h_buf, k_out, v_out,
                 ring, send_buf, recv_buf, n_buf, act_buf, kv_buf, q_buf, o_buf, again_buf, mgain_buf, tab_buf, cos_buf, sin_buf, m_sc, l_sc, acc_sc,
                 tab_sem, x_sem, wkv_sem, w_sem, kvs_sem, kvr_sem, ps_sem, pr_sem, ds_sem, dr_sem, free_sem):
    cp = lax.axis_index('cp')
    peer = {'tp': 1 - lax.axis_index('tp')}
    pair = {'cp': cp + 1 - 2 * lax.rem(cp, 2)}
    across = {'cp': lax.rem(cp + 2, 4)}
    tok, width = n_buf.shape
    n_blk = width // BLK
    n_gu = wg_ref.shape[1] // BLK
    n_q = wq_ref.shape[1] // BLK
    n_kv = wk_ref.shape[1] // HEAD_DIM
    groups = wq_ref.shape[1] // wk_ref.shape[1]
    n_chunk = tok // CHUNK
    stacked = groups * CHUNK
    gu_slots, d_slots = width // SLOT, wd_ref.shape[0] // SLOT
    gu_deep, d_deep = N_SLOT // (2 * gu_slots), N_SLOT // d_slots
    kv_slots = n_kv // 2 * gu_slots

    def ring_rows(slot, n):
        return pl.ds(pl.multiple_of(slot * SLOT, SLOT), n * SLOT)

    def load(src, slot, n):
        return pltpu.make_async_copy(src, ring.at[ring_rows(slot, n), :], w_sem.at[slot])

    def load_q(u):
        return load(wq_ref.at[:, at(u, BLK)], kv_slots + gu_slots * u, gu_slots)

    def load_wo(t):
        return load(wo_ref.at[:, at(lax.rem(t, n_blk), BLK)], lax.rem(t, N_SLOT), 1)

    def gate_slot(j):
        return lax.rem(j, gu_deep) * 2 * gu_slots

    def load_gate(j):
        return load(wg_ref.at[:, at(j, BLK)], gate_slot(j), gu_slots)

    def load_up(j):
        return load(wu_ref.at[:, at(j, BLK)], gate_slot(j) + gu_slots, gu_slots)

    def load_down(j):
        return load(wd_ref.at[:, at(j, BLK)], lax.rem(j, d_deep) * d_slots, d_slots)

    def load_kv(g, which):
        src = (wk_ref, wv_ref)[which]
        cols = at(lax.rem(g, 2) * 2 + which, HEAD_DIM)
        return pltpu.make_async_copy(src.at[:, at(g, HEAD_DIM)], ring.at[ring_rows(g // 2 * gu_slots, gu_slots), cols], wkv_sem.at[g, which])

    def load_x(i):
        return pltpu.make_async_copy(x_ref.at[at(i, X_ROWS), :], h_buf.at[at(i, X_ROWS), :], x_sem.at[i])

    def kv_copy(kind, g, r=0, n_rows=None):
        n_rows = n_rows or tok
        src_block = 2 if kind == 2 else 0
        rows = at(r, n_rows) if n_rows < tok else slice(None)
        return pltpu.make_async_remote_copy(kv_buf.at[src_block, g, rows, :], kv_buf.at[kind + 1, g, rows, :],
                                            kvs_sem.at[kind], kvr_sem.at[kind, g],
                                            device_id=across if kind == 1 else pair, device_id_type=MESH)

    def part_copy(i, j):
        piece = (j, at(i, CHUNK), slice(None))
        return pltpu.make_async_remote_copy(send_buf.at[piece], recv_buf.at[piece], ps_sem.at[i * CHUNK // HALF], pr_sem.at[i * CHUNK // HALF],
                                            device_id=peer, device_id_type=MESH)

    def down_copy(s, j):
        piece = (j, at(s, HALF), slice(None))
        return pltpu.make_async_remote_copy(send_buf.at[piece], recv_buf.at[piece], ds_sem.at[s], dr_sem.at[s, j],
                                            device_id=peer, device_id_type=MESH)

    def half_copy(s, sent_sem, got_sem):
        piece = (slice(None), at(s, HALF), slice(None))
        return pltpu.make_async_remote_copy(send_buf.at[piece], recv_buf.at[piece], sent_sem.at[s], got_sem,
                                            device_id=peer, device_id_type=MESH)

    def scale_rows(src_rows, dst_rows, total, gain_ref):
        inv = lax.rsqrt(jnp.sum(total, axis=-1, keepdims=True) / width + NORM_EPS)
        for r in range(width // LANES):
            cols = slice(r * LANES, (r + 1) * LANES)
            wide = h_buf[src_rows, cols].astype(F32)
            n_buf[dst_rows, cols] = (wide * inv * gain_ref[r:r + 1, :].astype(F32)).astype(BF)

    def rope(prod, rows):
        u = prod.astype(BF).astype(F32)
        return (u * cos_buf[rows, :] + pltpu.roll(u, HEAD_DIM // 2, 1) * sin_buf[rows, :]).astype(BF)

    small = [pltpu.make_async_copy(again_ref, again_buf, tab_sem.at[0]), pltpu.make_async_copy(mgain_ref, mgain_buf, tab_sem.at[1]),
             pltpu.make_async_copy(tab_ref.at[at(cp, tok), :], tab_buf, tab_sem.at[2])]
    for c in small:
        c.start()
    first_rows = 2 * KV_ROWS // X_ROWS
    loop(first_rows, lambda i: load_x(i).start())
    for g in range(2):
        for which in range(2):
            load_kv(g, which).start()
    lax.fori_loop(first_rows, tok // X_ROWS, lambda i, c: (load_x(i).start(), c)[1], 0)
    barrier = pltpu.get_barrier_semaphore()
    for other in (peer, pair, across):
        pl.semaphore_signal(barrier, inc=1, device_id=other, device_id_type=MESH)
    for c in small:
        c.wait()
    cos, sin = tab_buf[:, :HEAD_DIM // 2], tab_buf[:, HEAD_DIM // 2:]
    cos_buf[...] = jnp.concatenate([cos, cos], axis=1)
    sin_buf[...] = jnp.concatenate([-sin, sin], axis=1)

    def norm_step(i):
        load_x(i).wait()
        for part in range(X_ROWS // 32):
            rows = at(i * (X_ROWS // 32) + part, 32)
            total = jnp.zeros((32, BLK), F32)
            for j in range(n_blk):
                wide = h_buf[rows, j * BLK:(j + 1) * BLK].astype(F32)
                total += wide * wide
            scale_rows(rows, rows, total, again_buf)

    n_quarter = tok // KV_ROWS

    def kv_step(t):
        pair_heads, r = t // n_quarter, lax.rem(t, n_quarter)
        rows = at(r, KV_ROWS)

        @pl.when(t < n_quarter)
        def _():
            lax.fori_loop(r * (KV_ROWS // X_ROWS), (r + 1) * (KV_ROWS // X_ROWS), lambda i, c: (norm_step(i), c)[1], 0)

        @pl.when(t == 0)
        def _():
            pl.semaphore_wait(barrier, 3)

        @pl.when(t == 1)
        def _():
            for g in range(2, n_kv):
                for which in range(2):
                    load_kv(g, which).start()
            for u in range(n_q):
                load_q(u).start()

        @pl.when(r == 0)
        def _():
            for e in range(2):
                for which in range(2):
                    load_kv(2 * pair_heads + e, which).wait()
        prod = jnp.dot(n_buf[rows, :], ring[ring_rows(pair_heads * gu_slots, gu_slots), :], preferred_element_type=F32)
        for e in range(2):
            g = 2 * pair_heads + e
            col = e * 2 * HEAD_DIM
            kv_buf[0, g, rows, :HEAD_DIM] = rope(prod[:, col:col + HEAD_DIM], rows)
            kv_buf[0, g, rows, HEAD_DIM:] = prod[:, col + HEAD_DIM:col + 2 * HEAD_DIM].astype(BF)


        def send_kv(*piece):
            @pl.when(cp < 2)
            def _():
                kv_copy(1, *piece).start()

            @pl.when(lax.rem(cp, 2) == 0)
            def _():
                kv_copy(0, *piece).start()
        send_kv(2 * pair_heads, r, KV_ROWS)

        @pl.when(r == n_quarter - 1)
        def _():
            send_kv(2 * pair_heads + 1)
    loop(n_kv // 2 * n_quarter, kv_step)
    for t in range(kv_slots):
        load_wo(t).start()

    def q_step(u):
        load_q(u).wait()
        w = ring[ring_rows(kv_slots + gu_slots * u, gu_slots), :]
        prod = jnp.dot(n_buf[...], w, preferred_element_type=F32)
        for j in range(BLK // HEAD_DIM):
            q_buf[:, pl.ds(pl.multiple_of(u * BLK + j * HEAD_DIM, HEAD_DIM), HEAD_DIM)] = rope(prod[:, j * HEAD_DIM:(j + 1) * HEAD_DIM], slice(None))
        for t in range(gu_slots):
            load_wo(kv_slots + gu_slots * u + t).start()
    loop(n_q, q_step)

    lo = jnp.where(cp == 2, 2, 1)
    hi = jnp.where(cp == 0, 1, jnp.where(cp == 1, 2, 4))
    for i in range(n_chunk):
        row0 = i * CHUNK
        n_keys = row0 + CHUNK

        n_heads = 2

        def scores(g, b, n):
            q = jnp.concatenate([q_buf[row0:row0 + CHUNK, at(g * groups + j, HEAD_DIM)] for j in range(groups)], axis=0)
            return lax.dot_general(kv_buf[b, g, :n, :HEAD_DIM], q, (((1,), (1,)), ((), ())), preferred_element_type=F32)

        def weigh(g, b, n, p):
            return lax.dot_general(kv_buf[b, g, :n, HEAD_DIM:], p.astype(BF), (((0,), (0,)), ((), ())), preferred_element_type=F32)

        def pass_on(g):
            kv_copy(1, g).wait_recv()
            kv_copy(2, g).start()

        def head_step(step):
            heads = [step * n_heads + e for e in range(n_heads)]
            kpos = lax.broadcasted_iota(jnp.int32, (n_keys, stacked), 0)
            qpos = row0 + lax.rem(lax.broadcasted_iota(jnp.int32, (n_keys, stacked), 1), CHUNK)
            if i == 0:
                @pl.when(cp >= 2)
                def _():
                    pass_on(heads[0])
            all_s = [scores(g, 0, n_keys) for g in heads]
            for e, g in enumerate(heads):
                s = jnp.where(kpos <= qpos, all_s[e], MASK_VALUE)
                m0 = jnp.max(s, axis=0, keepdims=True)
                p = jnp.exp2(s * EXP2_SCALE - m0 * EXP2_SCALE)
                m_sc[e] = m0
                l_sc[e] = jnp.sum(p, axis=0, keepdims=True)
                acc_sc[e] = weigh(g, 0, n_keys, p)

            def block_step(b, c):
                if i == 0:
                    @pl.when(b == 1)
                    def _():
                        for g in heads:
                            kv_copy(0, g).wait_recv()

                    @pl.when(b == 2)
                    def _():
                        pass_on(heads[1])

                    @pl.when(b == 3)
                    def _():
                        for g in heads:
                            kv_copy(2, g).wait_recv()
                all_s = [scores(g, b, tok) for g in heads]
                for e, g in enumerate(heads):
                    s = all_s[e]
                    m_old = m_sc[e]
                    m_new = jnp.maximum(m_old, jnp.max(s, axis=0, keepdims=True))
                    alpha = jnp.exp2((m_old - m_new) * EXP2_SCALE)
                    p = jnp.exp2(s * EXP2_SCALE - m_new * EXP2_SCALE)
                    l_sc[e] = l_sc[e] * alpha + jnp.sum(p, axis=0, keepdims=True)
                    acc_sc[e] = acc_sc[e] * alpha + weigh(g, b, tok, p)
                    m_sc[e] = m_new
                return c
            lax.fori_loop(lo, hi, block_step, 0)
            for e, g in enumerate(heads):
                out = acc_sc[e] / l_sc[e]
                for j in range(groups):
                    o_buf[:, at(g * groups + j, HEAD_DIM)] = out[:, j * CHUNK:(j + 1) * CHUNK].T.astype(BF)
        loop(n_kv // n_heads, head_step)

        def wo_step(j):
            t = i * n_blk + j
            load_wo(t).wait()
            w = ring[ring_rows(lax.rem(t, N_SLOT), 1), :]
            send_buf[j, row0:row0 + CHUNK, :] = jnp.dot(o_buf[...], w, preferred_element_type=F32).astype(BF)
            part_copy(i, j).start()
            if (i + 1) * n_blk - 1 + N_SLOT < n_chunk * n_blk:
                load_wo(t + N_SLOT).start()
            else:
                @pl.when(t + N_SLOT < n_chunk * n_blk)
                def _():
                    load_wo(t + N_SLOT).start()

                first = n_chunk * n_blk - N_SLOT
                for b in range(gu_deep):
                    end = 2 * gu_slots * b
                    for which in range(2):
                        last_slot = end + which * gu_slots + gu_slots - 1
                        when = first + (last_slot - first) % N_SLOT

                        @pl.when(t == when)
                        def _():
                            (load_gate, load_up)[which](b).start()
        loop(n_blk, wo_step)

    def half_step(s):
        parts = half_copy(s, ps_sem, pr_sem.at[s])
        parts.wait_recv()
        parts.wait_send()

        def h_step(r):
            rows = at(s * (HALF // 32) + r, 32)
            total = jnp.zeros((32, BLK), F32)
            for j in range(n_blk):
                cols = slice(j * BLK, (j + 1) * BLK)
                add = send_buf[j, rows, :].astype(F32) + recv_buf[j, rows, :].astype(F32)
                h = (h_buf[rows, cols].astype(F32) + add).astype(BF)
                h_buf[rows, cols] = h
                wide = h.astype(F32)
                total += wide * wide
            scale_rows(rows, at(r, 32), total, mgain_buf)
        loop(HALF // 32, h_step)
        pl.semaphore_signal(free_sem.at[s], inc=1, device_id=peer, device_id_type=MESH)

        def gu_step(j):
            slot = gate_slot(j)
            load_gate(j).wait()
            gate = jnp.dot(n_buf[:HALF, :], ring[ring_rows(slot, gu_slots), :], preferred_element_type=F32)
            load_up(j).wait()
            up = jnp.dot(n_buf[:HALF, :], ring[ring_rows(slot + gu_slots, gu_slots), :], preferred_element_type=F32)
            act_buf[:, at(j, BLK)] = (gate / (1.0 + jnp.exp(-gate)) * up).astype(BF)

            @pl.when(j + gu_deep < n_gu)
            def _():
                load_gate(j + gu_deep).start()
                load_up(j + gu_deep).start()
            freed = 0
            for back in range(gu_deep, 0, -1):
                now = (2 * gu_slots * (gu_deep - back + 1)) // d_slots

                @pl.when(j == n_gu - back)
                def _():
                    for d in range(freed, now):
                        load_down(d).start()
                freed = now
        loop(n_gu, gu_step)
        pl.semaphore_wait(free_sem.at[s], 1)

        def down_step(j):
            load_down(j).wait()
            w = ring[ring_rows(lax.rem(j, d_deep) * d_slots, d_slots), :]
            send_buf[j, at(s, HALF), :] = jnp.dot(act_buf[...], w, preferred_element_type=F32).astype(BF)
            down_copy(s, j).start()

            @pl.when(j + d_deep < n_blk)
            def _():
                load_down(j + d_deep).start()
            freed = 0
            for back in range(d_deep, 0, -1):
                now = d_slots * (d_deep - back + 1) // gu_slots

                @pl.when((j == n_blk - back) & (s == 0))
                def _():
                    for d in range(freed, now):
                        (load_gate, load_up)[d % 2](d // 2).start()
                freed = now
        loop(n_blk, down_step)
    loop(tok // HALF, half_step)

    for g in range(n_kv):
        k_out[:, g, :] = kv_buf[0, g, :, :HEAD_DIM]
        v_out[:, g, :] = kv_buf[0, g, :, HEAD_DIM:]

    def final_step(t):
        s, j = t // n_blk, lax.rem(t, n_blk)
        down_copy(s, j).wait_recv()
        rows, cols = at(s, HALF), at(j, BLK)
        add = send_buf[j, rows, :].astype(F32) + recv_buf[j, rows, :].astype(F32)
        h_buf[rows, cols] = (h_buf[rows, cols].astype(F32) + add).astype(BF)
    loop(tok // HALF * n_blk, final_step)

    loop(tok // HALF, lambda s: half_copy(s, ds_sem, pr_sem.at[s]).wait_send())
    def kv_sent(kind):
        pltpu.make_async_remote_copy(kv_buf.at[0], kv_buf.at[kind + 1], kvs_sem.at[kind], kvr_sem.at[kind, 0],
                                     device_id=pair, device_id_type=MESH).wait_send()

    @pl.when(cp < 2)
    def _():
        kv_sent(1)

    @pl.when(lax.rem(cp, 2) == 0)
    def _():
        kv_sent(0)

    @pl.when(cp >= 2)
    def _():
        kv_sent(2)


def fused_layer(tab, attn_gain, mlp_gain, x, w_q, w_k, w_v, w_o, w_gate, w_up, w_down):
    tok, width = x.shape
    qcols, kcols, ff = w_q.shape[1], w_k.shape[1], w_gate.shape[1]
    n_blk, n_kv, halves = width // BLK, kcols // HEAD_DIM, tok // HALF
    stacked = CHUNK * (qcols // kcols)
    dma = pltpu.SemaphoreType.DMA
    return pl.pallas_call(
        layer_kernel,
        in_specs=[ANY] * 11,
        out_specs=[VMEM] * 3,
        out_shape=[pltpu.VMEM((tok, width), BF)] + [pltpu.VMEM((tok, n_kv, HEAD_DIM), BF)] * 2,
        scratch_shapes=[
            pltpu.VMEM((N_SLOT * SLOT, BLK), BF),
            pltpu.VMEM((n_blk, tok, BLK), BF), pltpu.VMEM((n_blk, tok, BLK), BF),
            pltpu.VMEM((tok, width), BF), pltpu.VMEM((HALF, ff), BF),
            pltpu.VMEM((4, n_kv, tok, 2 * HEAD_DIM), BF), pltpu.VMEM((tok, qcols), BF), pltpu.VMEM((CHUNK, qcols), BF),
            pltpu.VMEM((width // LANES, LANES), BF), pltpu.VMEM((width // LANES, LANES), BF),
            pltpu.VMEM((tok, HEAD_DIM), F32), pltpu.VMEM((tok, HEAD_DIM), F32), pltpu.VMEM((tok, HEAD_DIM), F32),
            pltpu.VMEM((2, 1, stacked), F32), pltpu.VMEM((2, 1, stacked), F32), pltpu.VMEM((2, HEAD_DIM, stacked), F32),
            dma((3,)), dma((tok // X_ROWS,)), dma((n_kv, 2)), dma((N_SLOT,)), dma((3,)), dma((3, n_kv)),
            dma((halves,)), dma((halves,)), dma((halves,)), dma((halves, n_blk)),
            pltpu.SemaphoreType.REGULAR((halves,))],
        compiler_params=pltpu.CompilerParams(vmem_limit_bytes=VMEM_LIMIT, collective_id=0, has_side_effects=True),
        name='fused_layer',
        cost_estimate=pl.CostEstimate(flops=2 * tok * width * (2 * qcols + 2 * kcols + 3 * ff), transcendentals=0,
                                      bytes_accessed=2 * width * (2 * qcols + 2 * kcols + 6 * ff)),
    )(tab, attn_gain, mlp_gain, x, w_q, w_k, w_v, w_o, w_gate, w_up, w_down)


def emit_kernel(y_ref, k_ref, v_ref, x_out, k_out, v_out, sem):
    copies = [pltpu.make_async_copy(y_ref.at[at(i, CHUNK), :], x_out.at[at(i, CHUNK), :], sem.at[i]) for i in range(y_ref.shape[0] // CHUNK)]
    copies += [pltpu.make_async_copy(k_ref, k_out, sem.at[len(copies)]), pltpu.make_async_copy(v_ref, v_out, sem.at[len(copies) + 1])]
    for c in copies:
        c.start()
    for c in copies:
        c.wait()


def emit(*results):
    here = [pltpu.with_memory_space_constraint(r, pltpu.VMEM) for r in results]
    return pl.pallas_call(
        emit_kernel, in_specs=[VMEM] * 3, out_specs=[ANY] * 3,
        out_shape=[jax.ShapeDtypeStruct(r.shape, r.dtype) for r in results],
        scratch_shapes=[pltpu.SemaphoreType.DMA((results[0].shape[0] // CHUNK + 2,))],
        compiler_params=pltpu.CompilerParams(vmem_limit_bytes=1 << 20), name='emit',
    )(*here)


def solution(mesh):
    row_spec = P(('dp', 'cp'), None)
    cache_spec = P(('dp', 'cp'), 'tp', None)
    col_spec = P(None, 'tp')
    split_rows = P('tp', None)
    vec_spec = P(None)

    def local_layer(x, attn_gain, w_q, w_k, w_v, w_o, mlp_gain, w_gate, w_up, w_down):
        tok, width = x.shape
        tab = jnp.asarray(rope_table(tok * mesh.shape['cp']))
        gains = [g.reshape(width // LANES, LANES) for g in (attn_gain, mlp_gain)]
        return tuple(emit(*fused_layer(tab, *gains, x, w_q, w_k, w_v, w_o, w_gate, w_up, w_down)))

    return jax.shard_map(local_layer, mesh=mesh,
                         in_specs=(row_spec, vec_spec, col_spec, col_spec, col_spec, split_rows, vec_spec, col_spec, col_spec, split_rows),
                         out_specs=(row_spec, cache_spec, cache_spec), check_vma=False)
```

```python
import jax
import jax.numpy as jnp
import numpy as np
from jax import lax
from jax.experimental import pallas as pl
from jax.experimental.pallas import tpu as pltpu
from jax.sharding import PartitionSpec as P

HEAD_DIM = 128
ROPE_THETA = 1000000.0
NORM_EPS = 1e-5
MASK_VALUE = -1e30
EXP2_SCALE = HEAD_DIM ** -0.5 * 1.4426950408889634
BF = jnp.bfloat16
F32 = jnp.float32
ANY = pl.BlockSpec(memory_space=pl.ANY)
VMEM = pl.BlockSpec(memory_space=pltpu.VMEM)
MESH = pl.DeviceIdType.MESH
LANES = 128
CHUNK = 128
HALF = 256
BLK = 512
SLOT = 2048
X_ROWS = 64
KV_ROWS = 128
N_RELAY = 2
N_SLOT = 12
VMEM_LIMIT = 60000000


def at(i, size):
    return pl.ds(pl.multiple_of(i * size, size), size)


def loop(n, body):
    def step(i, c):
        body(i)
        return c
    lax.fori_loop(0, n, step, 0)


def rope_table(n_pos):
    inv_freq = np.float32(ROPE_THETA) ** (-np.arange(0, HEAD_DIM, 2, dtype=np.float32) / np.float32(HEAD_DIM))
    angles = np.arange(n_pos, dtype=np.float32)[:, None] * inv_freq[None, :]
    return np.concatenate([np.cos(angles), np.sin(angles)], axis=1).astype(np.float32)


def layer_kernel(tab_ref, again_ref, mgain_ref, x_ref, wq_ref, wk_ref, wv_ref, wo_ref, wg_ref, wu_ref, wd_ref,
                 h_buf, k_out, v_out,
                 ring, send_buf, recv_buf, relay_buf, n_buf, act_buf, kv_buf, q_buf, o_buf, again_buf, mgain_buf, tab_buf, cos_buf, sin_buf, m_sc, l_sc, acc_sc,
                 tab_sem, x_sem, wkv_sem, w_sem, kvs_sem, kvr_sem, ps_sem, pr_sem, ds_sem, dr_sem, relay_sem, free_sem):
    cp = lax.axis_index('cp')
    peer = {'tp': 1 - lax.axis_index('tp')}
    pair = {'cp': cp + 1 - 2 * lax.rem(cp, 2)}
    across = {'cp': lax.rem(cp + 2, 4)}
    diagonal = {'tp': 1 - lax.axis_index('tp'), 'cp': lax.rem(cp + 2, 4)}
    tok, width = n_buf.shape
    n_blk = width // BLK
    n_gu = wg_ref.shape[1] // BLK
    n_q = wq_ref.shape[1] // BLK
    n_kv = wk_ref.shape[1] // HEAD_DIM
    groups = wq_ref.shape[1] // wk_ref.shape[1]
    n_chunk = tok // CHUNK
    stacked = groups * CHUNK
    gu_slots, d_slots = width // SLOT, wd_ref.shape[0] // SLOT
    gu_deep, d_deep = N_SLOT // (2 * gu_slots), N_SLOT // d_slots
    kv_slots = n_kv // 2 * gu_slots

    def ring_rows(slot, n):
        return pl.ds(pl.multiple_of(slot * SLOT, SLOT), n * SLOT)

    def load(src, slot, n):
        return pltpu.make_async_copy(src, ring.at[ring_rows(slot, n), :], w_sem.at[slot])

    def load_q(u):
        return load(wq_ref.at[:, at(u, BLK)], kv_slots + gu_slots * u, gu_slots)

    def wo_slot(t):
        return jnp.where(t < n_blk, lax.rem(t, kv_slots), lax.rem(t, N_SLOT))

    def load_wo(t):
        return load(wo_ref.at[:, at(lax.rem(t, n_blk), BLK)], wo_slot(t), 1)

    def gate_slot(j):
        return lax.rem(j, gu_deep) * 2 * gu_slots

    def load_gate(j):
        return load(wg_ref.at[:, at(j, BLK)], gate_slot(j), gu_slots)

    def load_up(j):
        return load(wu_ref.at[:, at(j, BLK)], gate_slot(j) + gu_slots, gu_slots)

    def load_down(j):
        return load(wd_ref.at[:, at(j, BLK)], lax.rem(j, d_deep) * d_slots, d_slots)

    def load_kv(u, which, part):
        src = (wk_ref, wv_ref)[which]
        rows = pl.ds(part * (width // 2), width // 2)
        dst = ring.at[pl.ds(u * gu_slots * SLOT + part * (width // 2), width // 2), pl.ds(which * 2 * HEAD_DIM, 2 * HEAD_DIM)]
        return pltpu.make_async_copy(src.at[rows, pl.ds(u * 2 * HEAD_DIM, 2 * HEAD_DIM)], dst, wkv_sem.at[u, which, part])

    def all_kv(u):
        return [load_kv(u, which, part) for part in range(2) for which in range(2)]

    def load_x(i):
        return pltpu.make_async_copy(x_ref.at[at(i, X_ROWS), :], h_buf.at[at(i, X_ROWS), :], x_sem.at[i])

    def kv_copy(kind, g, r=0, n_rows=None):
        n_rows = n_rows or tok
        src_block = 2 if kind == 2 else 0
        rows = at(r, n_rows) if n_rows < tok else slice(None)
        return pltpu.make_async_remote_copy(kv_buf.at[src_block, g, rows, :], kv_buf.at[kind + 1, g, rows, :],
                                            kvs_sem.at[kind], kvr_sem.at[kind, g],
                                            device_id=across if kind == 1 else pair, device_id_type=MESH)

    def part_copy(i, j):
        piece = (j, at(i, CHUNK), slice(None))
        return pltpu.make_async_remote_copy(send_buf.at[piece], recv_buf.at[piece], ps_sem.at[i * CHUNK // HALF], pr_sem.at[i * CHUNK // HALF],
                                            device_id=peer, device_id_type=MESH)

    def relay_piece(j):
        return (n_blk - N_RELAY + j, slice(0, CHUNK), slice(None))

    def relay_copy(j):
        return pltpu.make_async_remote_copy(send_buf.at[relay_piece(j)], relay_buf.at[j], ps_sem.at[0], relay_sem.at[0],
                                            device_id=diagonal, device_id_type=MESH)

    def forward_copy(j):
        return pltpu.make_async_remote_copy(relay_buf.at[j], recv_buf.at[relay_piece(j)], relay_sem.at[1], pr_sem.at[0],
                                            device_id=across, device_id_type=MESH)

    def down_copy(s, j):
        piece = (j, at(s, HALF), slice(None))
        return pltpu.make_async_remote_copy(send_buf.at[piece], recv_buf.at[piece], ds_sem.at[s], dr_sem.at[s, j],
                                            device_id=peer, device_id_type=MESH)

    def half_copy(s, sent_sem, got_sem):
        piece = (slice(None), at(s, HALF), slice(None))
        return pltpu.make_async_remote_copy(send_buf.at[piece], recv_buf.at[piece], sent_sem.at[s], got_sem,
                                            device_id=peer, device_id_type=MESH)

    def scale_rows(src_rows, dst_rows, total, gain_ref):
        inv = lax.rsqrt(jnp.sum(total, axis=-1, keepdims=True) / width + NORM_EPS)
        for r in range(width // LANES):
            cols = slice(r * LANES, (r + 1) * LANES)
            wide = h_buf[src_rows, cols].astype(F32)
            n_buf[dst_rows, cols] = (wide * inv * gain_ref[r:r + 1, :].astype(F32)).astype(BF)

    def rope(prod, rows):
        u = prod.astype(BF).astype(F32)
        return (u * cos_buf[rows, :] + pltpu.roll(u, HEAD_DIM // 2, 1) * sin_buf[rows, :]).astype(BF)

    barrier = pltpu.get_barrier_semaphore()
    for other in (peer, pair, across, diagonal):
        pl.semaphore_signal(barrier, inc=1, device_id=other, device_id_type=MESH)

    gain_copy = pltpu.make_async_copy(again_ref, again_buf, tab_sem.at[0])
    small = [pltpu.make_async_copy(mgain_ref, mgain_buf, tab_sem.at[1]), pltpu.make_async_copy(tab_ref.at[at(cp, tok), :], tab_buf, tab_sem.at[2])]
    gain_copy.start()
    first_rows = KV_ROWS // X_ROWS
    loop(first_rows, lambda i: load_x(i).start())
    for c in small + all_kv(0):
        c.start()
    lax.fori_loop(first_rows, tok // X_ROWS, lambda i, c: (load_x(i).start(), c)[1], 0)
    gain_copy.wait()

    def norm_step(i):
        load_x(i).wait()
        for part in range(X_ROWS // 32):
            rows = at(i * (X_ROWS // 32) + part, 32)
            total = jnp.zeros((32, BLK), F32)
            for j in range(n_blk):
                wide = h_buf[rows, j * BLK:(j + 1) * BLK].astype(F32)
                total += wide * wide
            scale_rows(rows, rows, total, again_buf)

    n_quarter = tok // KV_ROWS

    def kv_step(t):
        pair_heads, r = t // n_quarter, lax.rem(t, n_quarter)
        rows = at(r, KV_ROWS)

        @pl.when(t < n_quarter)
        def _():
            lax.fori_loop(r * (KV_ROWS // X_ROWS), (r + 1) * (KV_ROWS // X_ROWS), lambda i, c: (norm_step(i), c)[1], 0)

        @pl.when(t == 0)
        def _():
            for c in small:
                c.wait()
            cos, sin = tab_buf[:, :HEAD_DIM // 2], tab_buf[:, HEAD_DIM // 2:]
            cos_buf[...] = jnp.concatenate([cos, cos], axis=1)
            sin_buf[...] = jnp.concatenate([-sin, sin], axis=1)

        @pl.when(t == 1)
        def _():
            for u in range(1, n_kv // 2):
                for c in all_kv(u):
                    c.start()
            for u in range(n_q):
                load_q(u).start()

        @pl.when(r == 0)
        def _():
            for u in range(n_kv // 2):
                @pl.when(pair_heads == u)
                def _():
                    for c in all_kv(u):
                        c.wait()
        prod = jnp.dot(n_buf[rows, :], ring[ring_rows(pair_heads * gu_slots, gu_slots), :], preferred_element_type=F32)
        for e in range(2):
            g = 2 * pair_heads + e
            col = e * HEAD_DIM
            kv_buf[0, g, rows, :HEAD_DIM] = rope(prod[:, col:col + HEAD_DIM], rows)
            kv_buf[0, g, rows, HEAD_DIM:] = prod[:, col + 2 * HEAD_DIM:col + 3 * HEAD_DIM].astype(BF)


        @pl.when(t == 0)
        def _():
            pl.semaphore_wait(barrier, 4)

        def send_kv(*piece):
            @pl.when(cp < 2)
            def _():
                kv_copy(1, *piece).start()

            @pl.when(lax.rem(cp, 2) == 0)
            def _():
                kv_copy(0, *piece).start()
        send_kv(2 * pair_heads, r, KV_ROWS)

        @pl.when(r == n_quarter - 1)
        def _():
            send_kv(2 * pair_heads + 1)
    loop(n_kv // 2 * n_quarter, kv_step)
    for t in range(kv_slots):
        load_wo(t).start()

    def q_rows(u, row, n):
        w = ring[ring_rows(kv_slots + gu_slots * u, gu_slots), :]
        prod = jnp.dot(n_buf[row:row + n, :], w, preferred_element_type=F32)
        for j in range(BLK // HEAD_DIM):
            cols = pl.ds(pl.multiple_of(u * BLK + j * HEAD_DIM, HEAD_DIM), HEAD_DIM)
            q_buf[row:row + n, cols] = rope(prod[:, j * HEAD_DIM:(j + 1) * HEAD_DIM], slice(row, row + n))

    def q_first(u):
        load_q(u).wait()
        q_rows(u, 0, CHUNK)
    loop(n_q, q_first)

    def q_rest(u, c):
        q_rows(u, CHUNK, tok - CHUNK)
        for e in range(gu_slots):
            t = kv_slots + gu_slots * u + e
            load_wo(jnp.where(t < n_blk, t + N_SLOT, t)).start()
        return c
    q_early = jnp.where(cp >= 2, n_q - 1, 0)

    lo = jnp.where(cp == 2, 2, 1)
    hi = jnp.where(cp == 0, 1, jnp.where(cp == 1, 2, 4))
    for i in range(n_chunk):
        row0 = i * CHUNK
        n_keys = row0 + CHUNK

        n_heads = 2

        def scores(g, b, n):
            q = jnp.concatenate([q_buf[row0:row0 + CHUNK, at(g * groups + j, HEAD_DIM)] for j in range(groups)], axis=0)
            return lax.dot_general(kv_buf[b, g, :n, :HEAD_DIM], q, (((1,), (1,)), ((), ())), preferred_element_type=F32)

        def weigh(g, b, n, p):
            return lax.dot_general(kv_buf[b, g, :n, HEAD_DIM:], p.astype(BF), (((0,), (0,)), ((), ())), preferred_element_type=F32)

        def pass_on(g):
            kv_copy(1, g).wait_recv()
            kv_copy(2, g).start()

        def head_step(step):
            heads = [step * n_heads + e for e in range(n_heads)]
            kpos = lax.broadcasted_iota(jnp.int32, (n_keys, stacked), 0)
            qpos = row0 + lax.rem(lax.broadcasted_iota(jnp.int32, (n_keys, stacked), 1), CHUNK)
            if i == 0:
                @pl.when(cp >= 2)
                def _():
                    pass_on(heads[0])
            all_s = [scores(g, 0, n_keys) for g in heads]
            for e, g in enumerate(heads):
                s = jnp.where(kpos <= qpos, all_s[e], MASK_VALUE)
                m0 = jnp.max(s, axis=0, keepdims=True)
                p = jnp.exp2(s * EXP2_SCALE - m0 * EXP2_SCALE)
                m_sc[e] = m0
                l_sc[e] = jnp.sum(p, axis=0, keepdims=True)
                acc_sc[e] = weigh(g, 0, n_keys, p)

            def block_step(b, c):
                if i == 0:
                    @pl.when(b == 1)
                    def _():
                        for g in heads:
                            kv_copy(0, g).wait_recv()

                    @pl.when(b == 2)
                    def _():
                        pass_on(heads[1])

                    @pl.when(b == 3)
                    def _():
                        for g in heads:
                            kv_copy(2, g).wait_recv()
                all_s = [scores(g, b, tok) for g in heads]
                for e, g in enumerate(heads):
                    s = all_s[e]
                    m_old = m_sc[e]
                    m_new = jnp.maximum(m_old, jnp.max(s, axis=0, keepdims=True))
                    alpha = jnp.exp2((m_old - m_new) * EXP2_SCALE)
                    p = jnp.exp2(s * EXP2_SCALE - m_new * EXP2_SCALE)
                    l_sc[e] = l_sc[e] * alpha + jnp.sum(p, axis=0, keepdims=True)
                    acc_sc[e] = acc_sc[e] * alpha + weigh(g, b, tok, p)
                    m_sc[e] = m_new
                return c
            lax.fori_loop(lo, hi, block_step, 0)
            for e, g in enumerate(heads):
                out = acc_sc[e] / l_sc[e]
                for j in range(groups):
                    o_buf[:, at(g * groups + j, HEAD_DIM)] = out[:, j * CHUNK:(j + 1) * CHUNK].T.astype(BF)
            if i == 0:
                lax.fori_loop(jnp.where(step == 0, 0, q_early), q_early, q_rest, 0)
        loop(n_kv // n_heads, head_step)

        def wo_step(j):
            t = i * n_blk + j
            load_wo(t).wait()
            w = ring[ring_rows(wo_slot(t), 1), :]
            send_buf[j, row0:row0 + CHUNK, :] = jnp.dot(o_buf[...], w, preferred_element_type=F32).astype(BF)
            if i > 0:
                part_copy(i, j).start()
            else:
                relayed = (cp >= 2) & (j >= n_blk - N_RELAY)

                @pl.when(relayed)
                def _():
                    relay_copy(j - (n_blk - N_RELAY)).start()

                @pl.when(jnp.logical_not(relayed))
                def _():
                    part_copy(i, j).start()
            if i == 0:
                load_wo(jnp.where(j < kv_slots, t + kv_slots, t + n_blk)).start()
            elif (i + 1) * n_blk - 1 + N_SLOT < n_chunk * n_blk:
                load_wo(t + N_SLOT).start()
            else:
                @pl.when(t + N_SLOT < n_chunk * n_blk)
                def _():
                    load_wo(t + N_SLOT).start()

                first = n_chunk * n_blk - N_SLOT
                for b in range(gu_deep):
                    end = 2 * gu_slots * b
                    for which in range(2):
                        last_slot = end + which * gu_slots + gu_slots - 1
                        when = first + (last_slot - first) % N_SLOT

                        @pl.when(t == when)
                        def _():
                            (load_gate, load_up)[which](b).start()
        loop(n_blk, wo_step)
        if i == 0:
            lax.fori_loop(q_early, n_q, q_rest, 0)

    def half_step(s):
        @pl.when((s == 0) & (cp < 2))
        def _():
            pltpu.make_async_remote_copy(relay_buf, relay_buf, relay_sem.at[1], relay_sem.at[0], device_id=across, device_id_type=MESH).wait_recv()
            for j in range(N_RELAY):
                forward_copy(j).start()
        parts = half_copy(s, ps_sem, pr_sem.at[s])
        parts.wait_recv()
        parts.wait_send()

        def h_step(r):
            rows = at(s * (HALF // 32) + r, 32)
            total = jnp.zeros((32, BLK), F32)
            for j in range(n_blk):
                cols = slice(j * BLK, (j + 1) * BLK)
                add = send_buf[j, rows, :].astype(F32) + recv_buf[j, rows, :].astype(F32)
                h = (h_buf[rows, cols].astype(F32) + add).astype(BF)
                h_buf[rows, cols] = h
                wide = h.astype(F32)
                total += wide * wide
            scale_rows(rows, at(r, 32), total, mgain_buf)
        loop(HALF // 32, h_step)
        pl.semaphore_signal(free_sem.at[s], inc=1, device_id=peer, device_id_type=MESH)

        def gu_step(j):
            slot = gate_slot(j)
            load_gate(j).wait()
            gate = jnp.dot(n_buf[:HALF, :], ring[ring_rows(slot, gu_slots), :], preferred_element_type=F32)
            load_up(j).wait()
            up = jnp.dot(n_buf[:HALF, :], ring[ring_rows(slot + gu_slots, gu_slots), :], preferred_element_type=F32)
            act_buf[:, at(j, BLK)] = (gate / (1.0 + jnp.exp(-gate)) * up).astype(BF)

            @pl.when(j + gu_deep < n_gu)
            def _():
                load_gate(j + gu_deep).start()
                load_up(j + gu_deep).start()
            freed = 0
            for back in range(gu_deep, 0, -1):
                now = (2 * gu_slots * (gu_deep - back + 1)) // d_slots

                @pl.when(j == n_gu - back)
                def _():
                    for d in range(freed, now):
                        load_down(d).start()
                freed = now
        loop(n_gu, gu_step)
        pl.semaphore_wait(free_sem.at[s], 1)

        def down_step(j):
            load_down(j).wait()
            w = ring[ring_rows(lax.rem(j, d_deep) * d_slots, d_slots), :]
            send_buf[j, at(s, HALF), :] = jnp.dot(act_buf[...], w, preferred_element_type=F32).astype(BF)
            down_copy(s, j).start()

            @pl.when(j + d_deep < n_blk)
            def _():
                load_down(j + d_deep).start()
            freed = 0
            for back in range(d_deep, 0, -1):
                now = d_slots * (d_deep - back + 1) // gu_slots

                @pl.when((j == n_blk - back) & (s == 0))
                def _():
                    for d in range(freed, now):
                        (load_gate, load_up)[d % 2](d // 2).start()
                freed = now
        loop(n_blk, down_step)
    loop(tok // HALF, half_step)

    for g in range(n_kv):
        k_out[:, g, :] = kv_buf[0, g, :, :HEAD_DIM]
        v_out[:, g, :] = kv_buf[0, g, :, HEAD_DIM:]

    def final_step(t):
        s, j = t // n_blk, lax.rem(t, n_blk)
        down_copy(s, j).wait_recv()
        rows, cols = at(s, HALF), at(j, BLK)
        add = send_buf[j, rows, :].astype(F32) + recv_buf[j, rows, :].astype(F32)
        h_buf[rows, cols] = (h_buf[rows, cols].astype(F32) + add).astype(BF)
    loop(tok // HALF * n_blk, final_step)

    loop(tok // HALF, lambda s: half_copy(s, ds_sem, pr_sem.at[s]).wait_send())
    def kv_sent(kind):
        pltpu.make_async_remote_copy(kv_buf.at[0], kv_buf.at[kind + 1], kvs_sem.at[kind], kvr_sem.at[kind, 0],
                                     device_id=pair, device_id_type=MESH).wait_send()

    @pl.when(cp < 2)
    def _():
        kv_sent(1)
        pltpu.make_async_remote_copy(relay_buf, relay_buf, relay_sem.at[1], relay_sem.at[0], device_id=across, device_id_type=MESH).wait_send()

    @pl.when(lax.rem(cp, 2) == 0)
    def _():
        kv_sent(0)

    @pl.when(cp >= 2)
    def _():
        kv_sent(2)


def fused_layer(tab, attn_gain, mlp_gain, x, w_q, w_k, w_v, w_o, w_gate, w_up, w_down):
    tok, width = x.shape
    qcols, kcols, ff = w_q.shape[1], w_k.shape[1], w_gate.shape[1]
    n_blk, n_kv, halves = width // BLK, kcols // HEAD_DIM, tok // HALF
    stacked = CHUNK * (qcols // kcols)
    dma = pltpu.SemaphoreType.DMA
    return pl.pallas_call(
        layer_kernel,
        in_specs=[ANY] * 11,
        out_specs=[VMEM] * 3,
        out_shape=[pltpu.VMEM((tok, width), BF)] + [pltpu.VMEM((tok, n_kv, HEAD_DIM), BF)] * 2,
        scratch_shapes=[
            pltpu.VMEM((N_SLOT * SLOT, BLK), BF),
            pltpu.VMEM((n_blk, tok, BLK), BF), pltpu.VMEM((n_blk, tok, BLK), BF), pltpu.VMEM((N_RELAY, CHUNK, BLK), BF),
            pltpu.VMEM((tok, width), BF), pltpu.VMEM((HALF, ff), BF),
            pltpu.VMEM((4, n_kv, tok, 2 * HEAD_DIM), BF), pltpu.VMEM((tok, qcols), BF), pltpu.VMEM((CHUNK, qcols), BF),
            pltpu.VMEM((width // LANES, LANES), BF), pltpu.VMEM((width // LANES, LANES), BF),
            pltpu.VMEM((tok, HEAD_DIM), F32), pltpu.VMEM((tok, HEAD_DIM), F32), pltpu.VMEM((tok, HEAD_DIM), F32),
            pltpu.VMEM((2, 1, stacked), F32), pltpu.VMEM((2, 1, stacked), F32), pltpu.VMEM((2, HEAD_DIM, stacked), F32),
            dma((3,)), dma((tok // X_ROWS,)), dma((n_kv // 2, 2, 2)), dma((N_SLOT,)), dma((3,)), dma((3, n_kv)),
            dma((halves,)), dma((halves,)), dma((halves,)), dma((halves, n_blk)), dma((2,)),
            pltpu.SemaphoreType.REGULAR((halves,))],
        compiler_params=pltpu.CompilerParams(vmem_limit_bytes=VMEM_LIMIT, collective_id=0, has_side_effects=True),
        name='fused_layer',
        cost_estimate=pl.CostEstimate(flops=2 * tok * width * (2 * qcols + 2 * kcols + 3 * ff), transcendentals=0,
                                      bytes_accessed=2 * width * (2 * qcols + 2 * kcols + 6 * ff)),
    )(tab, attn_gain, mlp_gain, x, w_q, w_k, w_v, w_o, w_gate, w_up, w_down)


def emit_kernel(y_ref, k_ref, v_ref, x_out, k_out, v_out, sem):
    copies = [pltpu.make_async_copy(y_ref.at[at(i, CHUNK), :], x_out.at[at(i, CHUNK), :], sem.at[i]) for i in range(y_ref.shape[0] // CHUNK)]
    copies += [pltpu.make_async_copy(k_ref, k_out, sem.at[len(copies)]), pltpu.make_async_copy(v_ref, v_out, sem.at[len(copies) + 1])]
    for c in copies:
        c.start()
    for c in copies:
        c.wait()


def emit(*results):
    here = [pltpu.with_memory_space_constraint(r, pltpu.VMEM) for r in results]
    return pl.pallas_call(
        emit_kernel, in_specs=[VMEM] * 3, out_specs=[ANY] * 3,
        out_shape=[jax.ShapeDtypeStruct(r.shape, r.dtype) for r in results],
        scratch_shapes=[pltpu.SemaphoreType.DMA((results[0].shape[0] // CHUNK + 2,))],
        compiler_params=pltpu.CompilerParams(vmem_limit_bytes=1 << 20), name='emit',
    )(*here)


def solution(mesh):
    row_spec = P(('dp', 'cp'), None)
    cache_spec = P(('dp', 'cp'), 'tp', None)
    col_spec = P(None, 'tp')
    split_rows = P('tp', None)
    vec_spec = P(None)

    def local_layer(x, attn_gain, w_q, w_k, w_v, w_o, mlp_gain, w_gate, w_up, w_down):
        tok, width = x.shape
        tab = jnp.asarray(rope_table(tok * mesh.shape['cp']))
        gains = [g.reshape(width // LANES, LANES) for g in (attn_gain, mlp_gain)]
        return tuple(emit(*fused_layer(tab, *gains, x, w_q, w_k, w_v, w_o, w_gate, w_up, w_down)))

    return jax.shard_map(local_layer, mesh=mesh,
                         in_specs=(row_spec, vec_spec, col_spec, col_spec, col_spec, split_rows, vec_spec, col_spec, col_spec, split_rows),
                         out_specs=(row_spec, cache_spec, cache_spec), check_vma=False)
```

```python
import jax
import jax.numpy as jnp
import numpy as np
from jax import lax
from jax.experimental import pallas as pl
from jax.experimental.pallas import tpu as pltpu
from jax.sharding import PartitionSpec as P

HEAD_DIM = 128
ROPE_THETA = 1000000.0
NORM_EPS = 1e-5
MASK_VALUE = -1e30
EXP2_SCALE = HEAD_DIM ** -0.5 * 1.4426950408889634
BF = jnp.bfloat16
F32 = jnp.float32
ANY = pl.BlockSpec(memory_space=pl.ANY)
VMEM = pl.BlockSpec(memory_space=pltpu.VMEM)
MESH = pl.DeviceIdType.MESH
LANES = 128
CHUNK = 128
HALF = 256
BLK = 512
SLOT = 2048
X_ROWS = 64
KV_ROWS = 128
N_RELAY = 5
UNIT = 64
KV_PARTS = 2
N_SLOT = 12
VMEM_LIMIT = 60000000


def at(i, size):
    return pl.ds(pl.multiple_of(i * size, size), size)


def loop(n, body):
    def step(i, c):
        body(i)
        return c
    lax.fori_loop(0, n, step, 0)


def rope_table(n_pos):
    inv_freq = np.float32(ROPE_THETA) ** (-np.arange(0, HEAD_DIM, 2, dtype=np.float32) / np.float32(HEAD_DIM))
    angles = np.arange(n_pos, dtype=np.float32)[:, None] * inv_freq[None, :]
    return np.concatenate([np.cos(angles), np.sin(angles)], axis=1).astype(np.float32)


def layer_kernel(tab_ref, again_ref, mgain_ref, x_ref, wq_ref, wk_ref, wv_ref, wo_ref, wg_ref, wu_ref, wd_ref,
                 h_buf, k_out, v_out,
                 ring, send_buf, recv_buf, relay_buf, n_buf, act_buf, kv_buf, q_buf, o_buf, again_buf, mgain_buf, tab_buf, cos_buf, sin_buf, m_sc, l_sc, acc_sc,
                 tab_sem, x_sem, wkv_sem, w_sem, kvs_sem, kvr_sem, ps_sem, pr_sem, ds_sem, dr_sem, relay_sem, free_sem):
    cp = lax.axis_index('cp')
    peer = {'tp': 1 - lax.axis_index('tp')}
    pair = {'cp': cp + 1 - 2 * lax.rem(cp, 2)}
    across = {'cp': lax.rem(cp + 2, 4)}
    diagonal = {'tp': 1 - lax.axis_index('tp'), 'cp': lax.rem(cp + 2, 4)}
    tok, width = n_buf.shape
    n_blk = width // BLK
    n_gu = wg_ref.shape[1] // BLK
    n_q = wq_ref.shape[1] // BLK
    n_kv = wk_ref.shape[1] // HEAD_DIM
    groups = wq_ref.shape[1] // wk_ref.shape[1]
    n_chunk = tok // CHUNK
    stacked = groups * CHUNK
    gu_slots, d_slots = width // SLOT, wd_ref.shape[0] // SLOT
    gu_deep, d_deep = N_SLOT // (2 * gu_slots), N_SLOT // d_slots
    kv_slots = n_kv // 2 * gu_slots

    def ring_rows(slot, n):
        return pl.ds(pl.multiple_of(slot * SLOT, SLOT), n * SLOT)

    def load(src, slot, n):
        return pltpu.make_async_copy(src, ring.at[ring_rows(slot, n), :], w_sem.at[slot])

    def load_q(u):
        return load(wq_ref.at[:, at(u, BLK)], kv_slots + gu_slots * u, gu_slots)

    def wo_slot(t):
        return jnp.where(t < n_blk, lax.rem(t, kv_slots), lax.rem(t, N_SLOT))

    def load_wo(t):
        return load(wo_ref.at[:, at(lax.rem(t, n_blk), BLK)], wo_slot(t), 1)

    def gate_slot(j):
        return lax.rem(j, gu_deep) * 2 * gu_slots

    def load_gate(j):
        return load(wg_ref.at[:, at(j, BLK)], gate_slot(j), gu_slots)

    def load_up(j):
        return load(wu_ref.at[:, at(j, BLK)], gate_slot(j) + gu_slots, gu_slots)

    def load_down(j):
        return load(wd_ref.at[:, at(j, BLK)], lax.rem(j, d_deep) * d_slots, d_slots)

    def load_kv(u, which, part):
        src = (wk_ref, wv_ref)[which]
        n = width // KV_PARTS
        rows = pl.ds(part * n, n)
        dst = ring.at[pl.ds(u * gu_slots * SLOT + part * n, n), pl.ds(which * 2 * HEAD_DIM, 2 * HEAD_DIM)]
        return pltpu.make_async_copy(src.at[rows, pl.ds(u * 2 * HEAD_DIM, 2 * HEAD_DIM)], dst, wkv_sem.at[u, which, part])

    def all_kv(u):
        return [load_kv(u, which, part) for part in range(KV_PARTS) for which in range(2)]

    def load_x(i):
        return pltpu.make_async_copy(x_ref.at[at(i, X_ROWS), :], h_buf.at[at(i, X_ROWS), :], x_sem.at[i])

    def kv_copy(kind, g, r=0, n_rows=None):
        n_rows = n_rows or tok
        src_block = 2 if kind == 2 else 0
        rows = at(r, n_rows) if n_rows < tok else slice(None)
        return pltpu.make_async_remote_copy(kv_buf.at[src_block, g, rows, :], kv_buf.at[kind + 1, g, rows, :],
                                            kvs_sem.at[kind], kvr_sem.at[kind, g],
                                            device_id=across if kind == 1 else pair, device_id_type=MESH)

    def part_copy(i, j):
        piece = (j, at(i, CHUNK), slice(None))
        return pltpu.make_async_remote_copy(send_buf.at[piece], recv_buf.at[piece], ps_sem.at[i * CHUNK // HALF], pr_sem.at[i * CHUNK // HALF],
                                            device_id=peer, device_id_type=MESH)

    per_piece = CHUNK // UNIT
    first_relay = n_blk * per_piece - N_RELAY

    def unit(g):
        return (g // per_piece, at(lax.rem(g, per_piece), UNIT), slice(None))

    def unit_copy(g):
        return pltpu.make_async_remote_copy(send_buf.at[unit(g)], recv_buf.at[unit(g)], ps_sem.at[0], pr_sem.at[0],
                                            device_id=peer, device_id_type=MESH)

    def relay_copy(g):
        return pltpu.make_async_remote_copy(send_buf.at[unit(g)], relay_buf.at[g - first_relay], ps_sem.at[0], relay_sem.at[0],
                                            device_id=diagonal, device_id_type=MESH)

    def forward_copy(g):
        return pltpu.make_async_remote_copy(relay_buf.at[g - first_relay], recv_buf.at[unit(g)], relay_sem.at[1], pr_sem.at[0],
                                            device_id=across, device_id_type=MESH)

    def down_copy(s, j):
        piece = (j, at(s, HALF), slice(None))
        return pltpu.make_async_remote_copy(send_buf.at[piece], recv_buf.at[piece], ds_sem.at[s], dr_sem.at[s, j],
                                            device_id=peer, device_id_type=MESH)

    def half_copy(s, sent_sem, got_sem):
        piece = (slice(None), at(s, HALF), slice(None))
        return pltpu.make_async_remote_copy(send_buf.at[piece], recv_buf.at[piece], sent_sem.at[s], got_sem,
                                            device_id=peer, device_id_type=MESH)

    def scale_rows(src_rows, dst_rows, total, gain_ref):
        inv = lax.rsqrt(jnp.sum(total, axis=-1, keepdims=True) / width + NORM_EPS)
        for r in range(width // LANES):
            cols = slice(r * LANES, (r + 1) * LANES)
            wide = h_buf[src_rows, cols].astype(F32)
            n_buf[dst_rows, cols] = (wide * inv * gain_ref[r:r + 1, :].astype(F32)).astype(BF)

    def rope(prod, rows):
        u = prod.astype(BF).astype(F32)
        return (u * cos_buf[rows, :] + pltpu.roll(u, HEAD_DIM // 2, 1) * sin_buf[rows, :]).astype(BF)

    barrier = pltpu.get_barrier_semaphore()
    for other in (peer, pair, across, diagonal):
        pl.semaphore_signal(barrier, inc=1, device_id=other, device_id_type=MESH)

    gain_copy = pltpu.make_async_copy(again_ref, again_buf, tab_sem.at[0])
    small = [pltpu.make_async_copy(mgain_ref, mgain_buf, tab_sem.at[1]), pltpu.make_async_copy(tab_ref.at[at(cp, tok), :], tab_buf, tab_sem.at[2])]
    gain_copy.start()
    first_rows = KV_ROWS // X_ROWS
    loop(first_rows, lambda i: load_x(i).start())
    for c in small + all_kv(0):
        c.start()
    lax.fori_loop(first_rows, tok // X_ROWS, lambda i, c: (load_x(i).start(), c)[1], 0)
    gain_copy.wait()

    def norm_step(i):
        load_x(i).wait()
        for part in range(X_ROWS // 32):
            rows = at(i * (X_ROWS // 32) + part, 32)
            total = jnp.zeros((32, BLK), F32)
            for j in range(n_blk):
                wide = h_buf[rows, j * BLK:(j + 1) * BLK].astype(F32)
                total += wide * wide
            scale_rows(rows, rows, total, again_buf)

    n_quarter = tok // KV_ROWS

    def send_kv(*piece):
        @pl.when(cp < 2)
        def _():
            kv_copy(1, *piece).start()

        @pl.when(lax.rem(cp, 2) == 0)
        def _():
            kv_copy(0, *piece).start()

    def kv_rows(u, rows):
        prod = jnp.dot(n_buf[rows, :], ring[ring_rows(u * gu_slots, gu_slots), :], preferred_element_type=F32)
        for e in range(2):
            kv_buf[0, 2 * u + e, rows, :HEAD_DIM] = rope(prod[:, e * HEAD_DIM:(e + 1) * HEAD_DIM], rows)
            kv_buf[0, 2 * u + e, rows, HEAD_DIM:] = prod[:, (e + 2) * HEAD_DIM:(e + 3) * HEAD_DIM].astype(BF)

    def kv_step(r):
        lax.fori_loop(r * (KV_ROWS // X_ROWS), (r + 1) * (KV_ROWS // X_ROWS), lambda i, c: (norm_step(i), c)[1], 0)

        @pl.when(r == 0)
        def _():
            for c in small:
                c.wait()
            cos, sin = tab_buf[:, :HEAD_DIM // 2], tab_buf[:, HEAD_DIM // 2:]
            cos_buf[...] = jnp.concatenate([cos, cos], axis=1)
            sin_buf[...] = jnp.concatenate([-sin, sin], axis=1)
            for c in all_kv(0):
                c.wait()

        @pl.when(r == 1)
        def _():
            for u in range(1, n_kv // 2):
                for c in all_kv(u):
                    c.start()
            for u in range(n_q):
                load_q(u).start()
        kv_rows(0, at(r, KV_ROWS))

        @pl.when(r == 0)
        def _():
            pl.semaphore_wait(barrier, 4)
        send_kv(0, r, KV_ROWS)
    loop(n_quarter, kv_step)
    send_kv(1)
    for u in range(1, n_kv // 2):
        for c in all_kv(u):
            c.wait()
        kv_rows(u, slice(None))
        send_kv(2 * u)
        send_kv(2 * u + 1)
    for t in range(kv_slots):
        load_wo(t).start()

    def q_rows(u, row, n):
        w = ring[ring_rows(kv_slots + gu_slots * u, gu_slots), :]
        prod = jnp.dot(n_buf[row:row + n, :], w, preferred_element_type=F32)
        for j in range(BLK // HEAD_DIM):
            cols = pl.ds(pl.multiple_of(u * BLK + j * HEAD_DIM, HEAD_DIM), HEAD_DIM)
            q_buf[row:row + n, cols] = rope(prod[:, j * HEAD_DIM:(j + 1) * HEAD_DIM], slice(row, row + n))

    def q_first(u):
        load_q(u).wait()
        q_rows(u, 0, CHUNK)
    loop(n_q, q_first)

    def q_rest(u, c):
        q_rows(u, CHUNK, tok - CHUNK)
        for e in range(gu_slots):
            t = kv_slots + gu_slots * u + e
            load_wo(jnp.where(t < n_blk, t + N_SLOT, t)).start()
        return c
    q_early = jnp.where(cp >= 2, n_q - 1, 0)

    lo = jnp.where(cp == 2, 2, 1)
    hi = jnp.where(cp == 0, 1, jnp.where(cp == 1, 2, 4))
    for i in range(n_chunk):
        row0 = i * CHUNK
        n_keys = row0 + CHUNK

        n_heads = 2

        def scores(g, b, n):
            q = jnp.concatenate([q_buf[row0:row0 + CHUNK, at(g * groups + j, HEAD_DIM)] for j in range(groups)], axis=0)
            return lax.dot_general(kv_buf[b, g, :n, :HEAD_DIM], q, (((1,), (1,)), ((), ())), preferred_element_type=F32)

        def weigh(g, b, n, p):
            return lax.dot_general(kv_buf[b, g, :n, HEAD_DIM:], p.astype(BF), (((0,), (0,)), ((), ())), preferred_element_type=F32)

        def pass_on(g):
            kv_copy(1, g).wait_recv()
            kv_copy(2, g).start()

        def head_step(step):
            heads = [step * n_heads + e for e in range(n_heads)]
            kpos = lax.broadcasted_iota(jnp.int32, (n_keys, stacked), 0)
            qpos = row0 + lax.rem(lax.broadcasted_iota(jnp.int32, (n_keys, stacked), 1), CHUNK)
            if i == 0:
                @pl.when(cp >= 2)
                def _():
                    pass_on(heads[0])
            all_s = [scores(g, 0, n_keys) for g in heads]
            for e, g in enumerate(heads):
                s = jnp.where(kpos <= qpos, all_s[e], MASK_VALUE)
                m0 = jnp.max(s, axis=0, keepdims=True)
                p = jnp.exp2(s * EXP2_SCALE - m0 * EXP2_SCALE)
                m_sc[e] = m0
                l_sc[e] = jnp.sum(p, axis=0, keepdims=True)
                acc_sc[e] = weigh(g, 0, n_keys, p)

            def block_step(b, c):
                if i == 0:
                    @pl.when(b == 1)
                    def _():
                        for g in heads:
                            kv_copy(0, g).wait_recv()

                    @pl.when(b == 2)
                    def _():
                        pass_on(heads[1])

                    @pl.when(b == 3)
                    def _():
                        for g in heads:
                            kv_copy(2, g).wait_recv()
                all_s = [scores(g, b, tok) for g in heads]
                for e, g in enumerate(heads):
                    s = all_s[e]
                    m_old = m_sc[e]
                    m_new = jnp.maximum(m_old, jnp.max(s, axis=0, keepdims=True))
                    alpha = jnp.exp2((m_old - m_new) * EXP2_SCALE)
                    p = jnp.exp2(s * EXP2_SCALE - m_new * EXP2_SCALE)
                    l_sc[e] = l_sc[e] * alpha + jnp.sum(p, axis=0, keepdims=True)
                    acc_sc[e] = acc_sc[e] * alpha + weigh(g, b, tok, p)
                    m_sc[e] = m_new
                return c
            lax.fori_loop(lo, hi, block_step, 0)
            for e, g in enumerate(heads):
                out = acc_sc[e] / l_sc[e]
                for j in range(groups):
                    o_buf[:, at(g * groups + j, HEAD_DIM)] = out[:, j * CHUNK:(j + 1) * CHUNK].T.astype(BF)
            if i == 0:
                lax.fori_loop(jnp.where(step == 0, 0, q_early), q_early, q_rest, 0)
        loop(n_kv // n_heads, head_step)

        def wo_step(j):
            t = i * n_blk + j
            load_wo(t).wait()
            w = ring[ring_rows(wo_slot(t), 1), :]
            send_buf[j, row0:row0 + CHUNK, :] = jnp.dot(o_buf[...], w, preferred_element_type=F32).astype(BF)
            if i > 0:
                part_copy(i, j).start()
            else:
                @pl.when(cp < 2)
                def _():
                    part_copy(i, j).start()

                for e in range(per_piece):
                    g = j * per_piece + e

                    @pl.when((cp >= 2) & (g < first_relay))
                    def _():
                        unit_copy(g).start()

                    @pl.when((cp >= 2) & (g >= first_relay))
                    def _():
                        relay_copy(g).start()
            if i == 0:
                load_wo(jnp.where(j < kv_slots, t + kv_slots, t + n_blk)).start()
            elif (i + 1) * n_blk - 1 + N_SLOT < n_chunk * n_blk:
                load_wo(t + N_SLOT).start()
            else:
                @pl.when(t + N_SLOT < n_chunk * n_blk)
                def _():
                    load_wo(t + N_SLOT).start()

                first = n_chunk * n_blk - N_SLOT
                for b in range(gu_deep):
                    end = 2 * gu_slots * b
                    for which in range(2):
                        last_slot = end + which * gu_slots + gu_slots - 1
                        when = first + (last_slot - first) % N_SLOT

                        @pl.when(t == when)
                        def _():
                            (load_gate, load_up)[which](b).start()
        loop(n_blk, wo_step)
        if i == 0:
            lax.fori_loop(q_early, n_q, q_rest, 0)

    def half_step(s):
        @pl.when((s == 0) & (cp < 2))
        def _():
            pltpu.make_async_remote_copy(relay_buf, relay_buf, relay_sem.at[1], relay_sem.at[0], device_id=across, device_id_type=MESH).wait_recv()
            loop(N_RELAY, lambda k: forward_copy(first_relay + k).start())
        parts = half_copy(s, ps_sem, pr_sem.at[s])
        parts.wait_recv()
        parts.wait_send()

        def h_step(r):
            rows = at(s * (HALF // 32) + r, 32)
            total = jnp.zeros((32, BLK), F32)
            for j in range(n_blk):
                cols = slice(j * BLK, (j + 1) * BLK)
                add = send_buf[j, rows, :].astype(F32) + recv_buf[j, rows, :].astype(F32)
                h = (h_buf[rows, cols].astype(F32) + add).astype(BF)
                h_buf[rows, cols] = h
                wide = h.astype(F32)
                total += wide * wide
            scale_rows(rows, at(r, 32), total, mgain_buf)
        loop(HALF // 32, h_step)
        pl.semaphore_signal(free_sem.at[s], inc=1, device_id=peer, device_id_type=MESH)

        def gu_step(j):
            slot = gate_slot(j)
            load_gate(j).wait()
            gate = jnp.dot(n_buf[:HALF, :], ring[ring_rows(slot, gu_slots), :], preferred_element_type=F32)
            load_up(j).wait()
            up = jnp.dot(n_buf[:HALF, :], ring[ring_rows(slot + gu_slots, gu_slots), :], preferred_element_type=F32)
            act_buf[:, at(j, BLK)] = (gate / (1.0 + jnp.exp(-gate)) * up).astype(BF)

            @pl.when(j + gu_deep < n_gu)
            def _():
                load_gate(j + gu_deep).start()
                load_up(j + gu_deep).start()
            freed = 0
            for back in range(gu_deep, 0, -1):
                now = (2 * gu_slots * (gu_deep - back + 1)) // d_slots

                @pl.when(j == n_gu - back)
                def _():
                    for d in range(freed, now):
                        load_down(d).start()
                freed = now
        loop(n_gu, gu_step)
        pl.semaphore_wait(free_sem.at[s], 1)

        def down_step(j):
            load_down(j).wait()
            w = ring[ring_rows(lax.rem(j, d_deep) * d_slots, d_slots), :]
            send_buf[j, at(s, HALF), :] = jnp.dot(act_buf[...], w, preferred_element_type=F32).astype(BF)
            down_copy(s, j).start()

            @pl.when(j + d_deep < n_blk)
            def _():
                load_down(j + d_deep).start()
            freed = 0
            for back in range(d_deep, 0, -1):
                now = d_slots * (d_deep - back + 1) // gu_slots

                @pl.when((j == n_blk - back) & (s == 0))
                def _():
                    for d in range(freed, now):
                        (load_gate, load_up)[d % 2](d // 2).start()
                freed = now
        loop(n_blk, down_step)
    loop(tok // HALF, half_step)

    for g in range(n_kv):
        k_out[:, g, :] = kv_buf[0, g, :, :HEAD_DIM]
        v_out[:, g, :] = kv_buf[0, g, :, HEAD_DIM:]

    def final_step(t):
        s, j = t // n_blk, lax.rem(t, n_blk)
        down_copy(s, j).wait_recv()
        rows, cols = at(s, HALF), at(j, BLK)
        add = send_buf[j, rows, :].astype(F32) + recv_buf[j, rows, :].astype(F32)
        h_buf[rows, cols] = (h_buf[rows, cols].astype(F32) + add).astype(BF)
    loop(tok // HALF * n_blk, final_step)

    loop(tok // HALF, lambda s: half_copy(s, ds_sem, pr_sem.at[s]).wait_send())
    def kv_sent(kind):
        pltpu.make_async_remote_copy(kv_buf.at[0], kv_buf.at[kind + 1], kvs_sem.at[kind], kvr_sem.at[kind, 0],
                                     device_id=pair, device_id_type=MESH).wait_send()

    @pl.when(cp < 2)
    def _():
        kv_sent(1)
        pltpu.make_async_remote_copy(relay_buf, relay_buf, relay_sem.at[1], relay_sem.at[0], device_id=across, device_id_type=MESH).wait_send()

    @pl.when(lax.rem(cp, 2) == 0)
    def _():
        kv_sent(0)

    @pl.when(cp >= 2)
    def _():
        kv_sent(2)


def fused_layer(tab, attn_gain, mlp_gain, x, w_q, w_k, w_v, w_o, w_gate, w_up, w_down):
    tok, width = x.shape
    qcols, kcols, ff = w_q.shape[1], w_k.shape[1], w_gate.shape[1]
    n_blk, n_kv, halves = width // BLK, kcols // HEAD_DIM, tok // HALF
    stacked = CHUNK * (qcols // kcols)
    dma = pltpu.SemaphoreType.DMA
    return pl.pallas_call(
        layer_kernel,
        in_specs=[ANY] * 11,
        out_specs=[VMEM] * 3,
        out_shape=[pltpu.VMEM((tok, width), BF)] + [pltpu.VMEM((tok, n_kv, HEAD_DIM), BF)] * 2,
        scratch_shapes=[
            pltpu.VMEM((N_SLOT * SLOT, BLK), BF),
            pltpu.VMEM((n_blk, tok, BLK), BF), pltpu.VMEM((n_blk, tok, BLK), BF), pltpu.VMEM((N_RELAY, UNIT, BLK), BF),
            pltpu.VMEM((tok, width), BF), pltpu.VMEM((HALF, ff), BF),
            pltpu.VMEM((4, n_kv, tok, 2 * HEAD_DIM), BF), pltpu.VMEM((tok, qcols), BF), pltpu.VMEM((CHUNK, qcols), BF),
            pltpu.VMEM((width // LANES, LANES), BF), pltpu.VMEM((width // LANES, LANES), BF),
            pltpu.VMEM((tok, HEAD_DIM), F32), pltpu.VMEM((tok, HEAD_DIM), F32), pltpu.VMEM((tok, HEAD_DIM), F32),
            pltpu.VMEM((2, 1, stacked), F32), pltpu.VMEM((2, 1, stacked), F32), pltpu.VMEM((2, HEAD_DIM, stacked), F32),
            dma((3,)), dma((tok // X_ROWS,)), dma((n_kv // 2, 2, KV_PARTS)), dma((N_SLOT,)), dma((3,)), dma((3, n_kv)),
            dma((halves,)), dma((halves,)), dma((halves,)), dma((halves, n_blk)), dma((2,)),
            pltpu.SemaphoreType.REGULAR((halves,))],
        compiler_params=pltpu.CompilerParams(vmem_limit_bytes=VMEM_LIMIT, collective_id=0, has_side_effects=True),
        name='fused_layer',
        cost_estimate=pl.CostEstimate(flops=2 * tok * width * (2 * qcols + 2 * kcols + 3 * ff), transcendentals=0,
                                      bytes_accessed=2 * width * (2 * qcols + 2 * kcols + 6 * ff)),
    )(tab, attn_gain, mlp_gain, x, w_q, w_k, w_v, w_o, w_gate, w_up, w_down)


def emit_kernel(y_ref, k_ref, v_ref, x_out, k_out, v_out, sem):
    copies = [pltpu.make_async_copy(y_ref.at[at(i, CHUNK), :], x_out.at[at(i, CHUNK), :], sem.at[i]) for i in range(y_ref.shape[0] // CHUNK)]
    copies += [pltpu.make_async_copy(k_ref, k_out, sem.at[len(copies)]), pltpu.make_async_copy(v_ref, v_out, sem.at[len(copies) + 1])]
    for c in copies:
        c.start()
    for c in copies:
        c.wait()


def emit(*results):
    here = [pltpu.with_memory_space_constraint(r, pltpu.VMEM) for r in results]
    return pl.pallas_call(
        emit_kernel, in_specs=[VMEM] * 3, out_specs=[ANY] * 3,
        out_shape=[jax.ShapeDtypeStruct(r.shape, r.dtype) for r in results],
        scratch_shapes=[pltpu.SemaphoreType.DMA((results[0].shape[0] // CHUNK + 2,))],
        compiler_params=pltpu.CompilerParams(vmem_limit_bytes=1 << 20), name='emit',
    )(*here)


def solution(mesh):
    row_spec = P(('dp', 'cp'), None)
    cache_spec = P(('dp', 'cp'), 'tp', None)
    col_spec = P(None, 'tp')
    split_rows = P('tp', None)
    vec_spec = P(None)

    def local_layer(x, attn_gain, w_q, w_k, w_v, w_o, mlp_gain, w_gate, w_up, w_down):
        tok, width = x.shape
        tab = jnp.asarray(rope_table(tok * mesh.shape['cp']))
        gains = [g.reshape(width // LANES, LANES) for g in (attn_gain, mlp_gain)]
        return tuple(emit(*fused_layer(tab, *gains, x, w_q, w_k, w_v, w_o, w_gate, w_up, w_down)))

    return jax.shard_map(local_layer, mesh=mesh,
                         in_specs=(row_spec, vec_spec, col_spec, col_spec, col_spec, split_rows, vec_spec, col_spec, col_spec, split_rows),
                         out_specs=(row_spec, cache_spec, cache_spec), check_vma=False)
```

```python
import jax
import jax.numpy as jnp
import numpy as np
from jax import lax
from jax.experimental import pallas as pl
from jax.experimental.pallas import tpu as pltpu
from jax.sharding import PartitionSpec as P

HEAD_DIM = 128
ROPE_THETA = 1000000.0
NORM_EPS = 1e-5
MASK_VALUE = -1e30
EXP2_SCALE = HEAD_DIM ** -0.5 * 1.4426950408889634
BF = jnp.bfloat16
F32 = jnp.float32
ANY = pl.BlockSpec(memory_space=pl.ANY)
VMEM = pl.BlockSpec(memory_space=pltpu.VMEM)
MESH = pl.DeviceIdType.MESH
LANES = 128
CHUNK = 128
HALF = 256
BLK = 512
SLOT = 2048
X_ROWS = 64
KV_ROWS = 128
N_RELAY = 5
UNIT = 64
KV_PARTS = 2
N_SLOT = 12
VMEM_LIMIT = 60000000
EMIT_ROWS = 512


def at(i, size):
    return pl.ds(pl.multiple_of(i * size, size), size)


def loop(n, body):
    def step(i, c):
        body(i)
        return c
    lax.fori_loop(0, n, step, 0)


def rope_table(n_pos):
    inv_freq = np.float32(ROPE_THETA) ** (-np.arange(0, HEAD_DIM, 2, dtype=np.float32) / np.float32(HEAD_DIM))
    angles = np.arange(n_pos, dtype=np.float32)[:, None] * inv_freq[None, :]
    return np.concatenate([np.cos(angles), np.sin(angles)], axis=1).astype(np.float32)


def layer_kernel(tab_ref, again_ref, mgain_ref, x_ref, wq_ref, wk_ref, wv_ref, wo_ref, wg_ref, wu_ref, wd_ref,
                 h_buf, k_out, v_out,
                 ring, send_buf, recv_buf, relay_buf, n_buf, act_buf, kv_buf, q_buf, o_buf, again_buf, mgain_buf, tab_buf, cos_buf, sin_buf, m_sc, l_sc, acc_sc,
                 tab_sem, x_sem, wkv_sem, w_sem, kvs_sem, kvr_sem, ps_sem, pr_sem, ds_sem, dr_sem, relay_sem, free_sem):
    cp = lax.axis_index('cp')
    peer = {'tp': 1 - lax.axis_index('tp')}
    pair = {'cp': cp + 1 - 2 * lax.rem(cp, 2)}
    across = {'cp': lax.rem(cp + 2, 4)}
    diagonal = {'tp': 1 - lax.axis_index('tp'), 'cp': lax.rem(cp + 2, 4)}
    tok, width = n_buf.shape
    n_blk = width // BLK
    n_gu = wg_ref.shape[1] // BLK
    n_q = wq_ref.shape[1] // BLK
    n_kv = wk_ref.shape[1] // HEAD_DIM
    groups = wq_ref.shape[1] // wk_ref.shape[1]
    n_chunk = tok // CHUNK
    stacked = groups * CHUNK
    gu_slots, d_slots = width // SLOT, wd_ref.shape[0] // SLOT
    gu_deep, d_deep = N_SLOT // (2 * gu_slots), N_SLOT // d_slots
    kv_slots = n_kv // 2 * gu_slots

    def ring_rows(slot, n):
        return pl.ds(pl.multiple_of(slot * SLOT, SLOT), n * SLOT)

    def load(src, slot, n):
        return pltpu.make_async_copy(src, ring.at[ring_rows(slot, n), :], w_sem.at[slot])

    def load_q(u):
        return load(wq_ref.at[:, at(u, BLK)], kv_slots + gu_slots * u, gu_slots)

    def wo_slot(t):
        return jnp.where(t < n_blk, lax.rem(t, kv_slots), lax.rem(t, N_SLOT))

    def load_wo(t):
        return load(wo_ref.at[:, at(lax.rem(t, n_blk), BLK)], wo_slot(t), 1)

    def gate_slot(j):
        return lax.rem(j, gu_deep) * 2 * gu_slots

    def load_gate(j):
        return load(wg_ref.at[:, at(j, BLK)], gate_slot(j), gu_slots)

    def load_up(j):
        return load(wu_ref.at[:, at(j, BLK)], gate_slot(j) + gu_slots, gu_slots)

    def load_down(j):
        return load(wd_ref.at[:, at(j, BLK)], lax.rem(j, d_deep) * d_slots, d_slots)

    def load_kv(u, which, part):
        src = (wk_ref, wv_ref)[which]
        n = width // KV_PARTS
        rows = pl.ds(part * n, n)
        dst = ring.at[pl.ds(u * gu_slots * SLOT + part * n, n), pl.ds(which * 2 * HEAD_DIM, 2 * HEAD_DIM)]
        return pltpu.make_async_copy(src.at[rows, pl.ds(u * 2 * HEAD_DIM, 2 * HEAD_DIM)], dst, wkv_sem.at[u, which, part])

    def all_kv(u):
        return [load_kv(u, which, part) for part in range(KV_PARTS) for which in range(2)]

    def load_x(i):
        return pltpu.make_async_copy(x_ref.at[at(i, X_ROWS), :], h_buf.at[at(i, X_ROWS), :], x_sem.at[i])

    def kv_copy(kind, g, r=0, n_rows=None):
        n_rows = n_rows or tok
        src_block = 2 if kind == 2 else 0
        rows = at(r, n_rows) if n_rows < tok else slice(None)
        return pltpu.make_async_remote_copy(kv_buf.at[src_block, g, rows, :], kv_buf.at[kind + 1, g, rows, :],
                                            kvs_sem.at[kind], kvr_sem.at[kind, g],
                                            device_id=across if kind == 1 else pair, device_id_type=MESH)

    def kv_half(kind, g, r):
        src_block = 2 if kind == 2 else 0
        rows = pl.ds(r * HALF, HALF)
        return pltpu.make_async_remote_copy(kv_buf.at[src_block, g, rows, :], kv_buf.at[kind + 1, g, rows, :],
                                            kvs_sem.at[kind], kvr_sem.at[kind if kind == 2 or r == 0 else 3, g],
                                            device_id=across if kind == 1 else pair, device_id_type=MESH)

    def part_copy(i, j):
        piece = (j, at(i, CHUNK), slice(None))
        return pltpu.make_async_remote_copy(send_buf.at[piece], recv_buf.at[piece], ps_sem.at[i * CHUNK // HALF], pr_sem.at[i * CHUNK // HALF],
                                            device_id=peer, device_id_type=MESH)

    per_piece = CHUNK // UNIT
    first_relay = n_blk * per_piece - N_RELAY

    def unit(g):
        return (g // per_piece, at(lax.rem(g, per_piece), UNIT), slice(None))

    def unit_copy(g):
        return pltpu.make_async_remote_copy(send_buf.at[unit(g)], recv_buf.at[unit(g)], ps_sem.at[0], pr_sem.at[0],
                                            device_id=peer, device_id_type=MESH)

    def relay_copy(g):
        return pltpu.make_async_remote_copy(send_buf.at[unit(g)], relay_buf.at[g - first_relay], ps_sem.at[0], relay_sem.at[0],
                                            device_id=diagonal, device_id_type=MESH)

    def forward_copy(g):
        return pltpu.make_async_remote_copy(relay_buf.at[g - first_relay], recv_buf.at[unit(g)], relay_sem.at[1], pr_sem.at[0],
                                            device_id=across, device_id_type=MESH)

    def down_copy(s, j):
        piece = (j, at(s, HALF), slice(None))
        return pltpu.make_async_remote_copy(send_buf.at[piece], recv_buf.at[piece], ds_sem.at[s], dr_sem.at[s, j],
                                            device_id=peer, device_id_type=MESH)

    def half_copy(s, sent_sem, got_sem):
        piece = (slice(None), at(s, HALF), slice(None))
        return pltpu.make_async_remote_copy(send_buf.at[piece], recv_buf.at[piece], sent_sem.at[s], got_sem,
                                            device_id=peer, device_id_type=MESH)

    def scale_rows(src_rows, dst_rows, total, gain_ref):
        inv = lax.rsqrt(jnp.sum(total, axis=-1, keepdims=True) / width + NORM_EPS)
        for r in range(width // LANES):
            cols = slice(r * LANES, (r + 1) * LANES)
            wide = h_buf[src_rows, cols].astype(F32)
            n_buf[dst_rows, cols] = (wide * inv * gain_ref[r:r + 1, :].astype(F32)).astype(BF)

    def rope(prod, rows):
        u = prod.astype(BF).astype(F32)
        return (u * cos_buf[rows, :] + pltpu.roll(u, HEAD_DIM // 2, 1) * sin_buf[rows, :]).astype(BF)

    barrier = pltpu.get_barrier_semaphore()
    for other in (peer, pair, across, diagonal):
        pl.semaphore_signal(barrier, inc=1, device_id=other, device_id_type=MESH)

    gain_copy = pltpu.make_async_copy(again_ref, again_buf, tab_sem.at[0])
    small = [pltpu.make_async_copy(mgain_ref, mgain_buf, tab_sem.at[1]), pltpu.make_async_copy(tab_ref.at[at(cp, tok), :], tab_buf, tab_sem.at[2])]
    gain_copy.start()
    first_rows = KV_ROWS // X_ROWS
    loop(first_rows, lambda i: load_x(i).start())
    for c in small + all_kv(0):
        c.start()
    lax.fori_loop(first_rows, tok // X_ROWS, lambda i, c: (load_x(i).start(), c)[1], 0)
    gain_copy.wait()

    def norm_step(i):
        load_x(i).wait()
        for part in range(X_ROWS // 32):
            rows = at(i * (X_ROWS // 32) + part, 32)
            total = jnp.zeros((32, BLK), F32)
            for j in range(n_blk):
                wide = h_buf[rows, j * BLK:(j + 1) * BLK].astype(F32)
                total += wide * wide
            scale_rows(rows, rows, total, again_buf)

    n_quarter = tok // KV_ROWS

    def send_kv(*piece):
        @pl.when(cp < 2)
        def _():
            if len(piece) == 1 and piece[0] % 2:
                for r in range(tok // HALF):
                    kv_half(1, piece[0], r).start()
            else:
                kv_copy(1, *piece).start()

        @pl.when(lax.rem(cp, 2) == 0)
        def _():
            kv_copy(0, *piece).start()

    def kv_rows(u, rows):
        prod = jnp.dot(n_buf[rows, :], ring[ring_rows(u * gu_slots, gu_slots), :], preferred_element_type=F32)
        for e in range(2):
            kv_buf[0, 2 * u + e, rows, :HEAD_DIM] = rope(prod[:, e * HEAD_DIM:(e + 1) * HEAD_DIM], rows)
            kv_buf[0, 2 * u + e, rows, HEAD_DIM:] = prod[:, (e + 2) * HEAD_DIM:(e + 3) * HEAD_DIM].astype(BF)

    def kv_step(r):
        lax.fori_loop(r * (KV_ROWS // X_ROWS), (r + 1) * (KV_ROWS // X_ROWS), lambda i, c: (norm_step(i), c)[1], 0)

        @pl.when(r == 0)
        def _():
            for c in small:
                c.wait()
            cos, sin = tab_buf[:, :HEAD_DIM // 2], tab_buf[:, HEAD_DIM // 2:]
            cos_buf[...] = jnp.concatenate([cos, cos], axis=1)
            sin_buf[...] = jnp.concatenate([-sin, sin], axis=1)
            for c in all_kv(0):
                c.wait()

        @pl.when(r == 1)
        def _():
            for u in range(1, n_kv // 2):
                for c in all_kv(u):
                    c.start()
            for u in range(n_q):
                load_q(u).start()
        kv_rows(0, at(r, KV_ROWS))

        @pl.when(r == 0)
        def _():
            pl.semaphore_wait(barrier, 4)
        send_kv(0, r, KV_ROWS)
    loop(n_quarter, kv_step)
    send_kv(1)
    for u in range(1, n_kv // 2):
        for c in all_kv(u):
            c.wait()
        kv_rows(u, slice(None))
        send_kv(2 * u)
        send_kv(2 * u + 1)
    for t in range(kv_slots):
        load_wo(t).start()

    def q_rows(u, row, n):
        w = ring[ring_rows(kv_slots + gu_slots * u, gu_slots), :]
        prod = jnp.dot(n_buf[row:row + n, :], w, preferred_element_type=F32)
        for j in range(BLK // HEAD_DIM):
            cols = pl.ds(pl.multiple_of(u * BLK + j * HEAD_DIM, HEAD_DIM), HEAD_DIM)
            q_buf[row:row + n, cols] = rope(prod[:, j * HEAD_DIM:(j + 1) * HEAD_DIM], slice(row, row + n))

    def q_first(u):
        load_q(u).wait()
        q_rows(u, 0, CHUNK)
    loop(n_q, q_first)

    def q_rest(u, c):
        q_rows(u, CHUNK, tok - CHUNK)
        for e in range(gu_slots):
            t = kv_slots + gu_slots * u + e
            load_wo(jnp.where(t < n_blk, t + N_SLOT, t)).start()
        return c
    q_early = jnp.where(cp >= 2, n_q - 2, 0)

    lo = jnp.where(cp == 2, 2, 1)
    hi = jnp.where(cp == 0, 1, jnp.where(cp == 1, 2, 4))
    for i in range(n_chunk):
        row0 = i * CHUNK
        n_keys = row0 + CHUNK

        n_heads = 2

        def scores(g, b, n):
            q = jnp.concatenate([q_buf[row0:row0 + CHUNK, at(g * groups + j, HEAD_DIM)] for j in range(groups)], axis=0)
            return lax.dot_general(kv_buf[b, g, :n, :HEAD_DIM], q, (((1,), (1,)), ((), ())), preferred_element_type=F32)

        def weigh(g, b, n, p):
            return lax.dot_general(kv_buf[b, g, :n, HEAD_DIM:], p.astype(BF), (((0,), (0,)), ((), ())), preferred_element_type=F32)

        def pass_on(g):
            kv_copy(1, g).wait_recv()
            kv_copy(2, g).start()

        def head_step(step):
            heads = [step * n_heads + e for e in range(n_heads)]
            kpos = lax.broadcasted_iota(jnp.int32, (n_keys, stacked), 0)
            qpos = row0 + lax.rem(lax.broadcasted_iota(jnp.int32, (n_keys, stacked), 1), CHUNK)
            if i == 0:
                @pl.when(cp >= 2)
                def _():
                    pass_on(heads[0])
            all_s = [scores(g, 0, n_keys) for g in heads]
            for e, g in enumerate(heads):
                s = jnp.where(kpos <= qpos, all_s[e], MASK_VALUE)
                m0 = jnp.max(s, axis=0, keepdims=True)
                p = jnp.exp2(s * EXP2_SCALE - m0 * EXP2_SCALE)
                m_sc[e] = m0
                l_sc[e] = jnp.sum(p, axis=0, keepdims=True)
                acc_sc[e] = weigh(g, 0, n_keys, p)

            def block_step(b, c):
                if i == 0:
                    @pl.when(b == 1)
                    def _():
                        for g in heads:
                            kv_copy(0, g).wait_recv()

                    @pl.when(b == 2)
                    def _():
                        for r in range(tok // HALF):
                            kv_half(1, heads[1], r).wait_recv()
                            kv_half(2, heads[1], r).start()

                    @pl.when(b == 3)
                    def _():
                        for g in heads:
                            kv_copy(2, g).wait_recv()
                all_s = [scores(g, b, tok) for g in heads]
                for e, g in enumerate(heads):
                    s = all_s[e]
                    m_old = m_sc[e]
                    m_new = jnp.maximum(m_old, jnp.max(s, axis=0, keepdims=True))
                    alpha = jnp.exp2((m_old - m_new) * EXP2_SCALE)
                    p = jnp.exp2(s * EXP2_SCALE - m_new * EXP2_SCALE)
                    l_sc[e] = l_sc[e] * alpha + jnp.sum(p, axis=0, keepdims=True)
                    acc_sc[e] = acc_sc[e] * alpha + weigh(g, b, tok, p)
                    m_sc[e] = m_new
                return c
            lax.fori_loop(lo, hi, block_step, 0)
            for e, g in enumerate(heads):
                out = acc_sc[e] / l_sc[e]
                for j in range(groups):
                    o_buf[:, at(g * groups + j, HEAD_DIM)] = out[:, j * CHUNK:(j + 1) * CHUNK].T.astype(BF)
            if i == 0:
                lax.fori_loop(jnp.where(step == 0, 0, q_early), q_early, q_rest, 0)
        loop(n_kv // n_heads, head_step)

        def wo_step(j):
            t = i * n_blk + j
            load_wo(t).wait()
            w = ring[ring_rows(wo_slot(t), 1), :]
            send_buf[j, row0:row0 + CHUNK, :] = jnp.dot(o_buf[...], w, preferred_element_type=F32).astype(BF)
            if i > 0:
                part_copy(i, j).start()
            else:
                @pl.when(cp < 2)
                def _():
                    part_copy(i, j).start()

                for e in range(per_piece):
                    g = j * per_piece + e

                    @pl.when((cp >= 2) & (g < first_relay))
                    def _():
                        unit_copy(g).start()

                    @pl.when((cp >= 2) & (g >= first_relay))
                    def _():
                        relay_copy(g).start()
            if i == 0:
                load_wo(jnp.where(j < kv_slots, t + kv_slots, t + n_blk)).start()
            elif (i + 1) * n_blk - 1 + N_SLOT < n_chunk * n_blk:
                load_wo(t + N_SLOT).start()
            else:
                @pl.when(t + N_SLOT < n_chunk * n_blk)
                def _():
                    load_wo(t + N_SLOT).start()

                first = n_chunk * n_blk - N_SLOT
                for b in range(gu_deep):
                    end = 2 * gu_slots * b
                    for which in range(2):
                        last_slot = end + which * gu_slots + gu_slots - 1
                        when = first + (last_slot - first) % N_SLOT

                        @pl.when(t == when)
                        def _():
                            (load_gate, load_up)[which](b).start()
        loop(n_blk, wo_step)
        if i == 0:
            lax.fori_loop(q_early, n_q, q_rest, 0)

    def half_step(s):
        @pl.when((s == 0) & (cp < 2))
        def _():
            pltpu.make_async_remote_copy(relay_buf, relay_buf, relay_sem.at[1], relay_sem.at[0], device_id=across, device_id_type=MESH).wait_recv()
            loop(N_RELAY, lambda k: forward_copy(first_relay + k).start())
        parts = half_copy(s, ps_sem, pr_sem.at[s])
        parts.wait_recv()
        parts.wait_send()

        def h_step(r):
            rows = at(s * (HALF // 32) + r, 32)
            total = jnp.zeros((32, BLK), F32)
            for j in range(n_blk):
                cols = slice(j * BLK, (j + 1) * BLK)
                add = send_buf[j, rows, :].astype(F32) + recv_buf[j, rows, :].astype(F32)
                h = (h_buf[rows, cols].astype(F32) + add).astype(BF)
                h_buf[rows, cols] = h
                wide = h.astype(F32)
                total += wide * wide
            scale_rows(rows, at(r, 32), total, mgain_buf)
        loop(HALF // 32, h_step)
        pl.semaphore_signal(free_sem.at[s], inc=1, device_id=peer, device_id_type=MESH)

        def gu_step(j):
            slot = gate_slot(j)
            load_gate(j).wait()
            gate = jnp.dot(n_buf[:HALF, :], ring[ring_rows(slot, gu_slots), :], preferred_element_type=F32)
            load_up(j).wait()
            up = jnp.dot(n_buf[:HALF, :], ring[ring_rows(slot + gu_slots, gu_slots), :], preferred_element_type=F32)
            act_buf[:, at(j, BLK)] = (gate / (1.0 + jnp.exp(-gate)) * up).astype(BF)

            @pl.when(j + gu_deep < n_gu)
            def _():
                load_gate(j + gu_deep).start()
                load_up(j + gu_deep).start()
            freed = 0
            for back in range(gu_deep, 0, -1):
                now = (2 * gu_slots * (gu_deep - back + 1)) // d_slots

                @pl.when(j == n_gu - back)
                def _():
                    for d in range(freed, now):
                        load_down(d).start()
                freed = now
        loop(n_gu, gu_step)
        pl.semaphore_wait(free_sem.at[s], 1)

        def down_step(j):
            load_down(j).wait()
            w = ring[ring_rows(lax.rem(j, d_deep) * d_slots, d_slots), :]
            send_buf[j, at(s, HALF), :] = jnp.dot(act_buf[...], w, preferred_element_type=F32).astype(BF)
            down_copy(s, j).start()

            @pl.when(j + d_deep < n_blk)
            def _():
                load_down(j + d_deep).start()
            freed = 0
            for back in range(d_deep, 0, -1):
                now = d_slots * (d_deep - back + 1) // gu_slots

                @pl.when((j == n_blk - back) & (s == 0))
                def _():
                    for d in range(freed, now):
                        (load_gate, load_up)[d % 2](d // 2).start()
                freed = now
        loop(n_blk, down_step)
    loop(tok // HALF, half_step)

    for g in range(n_kv):
        k_out[:, g, :] = kv_buf[0, g, :, :HEAD_DIM]
        v_out[:, g, :] = kv_buf[0, g, :, HEAD_DIM:]

    def final_step(t):
        s, j = t // n_blk, lax.rem(t, n_blk)
        down_copy(s, j).wait_recv()
        rows, cols = at(s, HALF), at(j, BLK)
        add = send_buf[j, rows, :].astype(F32) + recv_buf[j, rows, :].astype(F32)
        h_buf[rows, cols] = (h_buf[rows, cols].astype(F32) + add).astype(BF)
    loop(tok // HALF * n_blk, final_step)

    loop(tok // HALF, lambda s: half_copy(s, ds_sem, pr_sem.at[s]).wait_send())
    def kv_sent(kind):
        pltpu.make_async_remote_copy(kv_buf.at[0], kv_buf.at[kind + 1], kvs_sem.at[kind], kvr_sem.at[kind, 0],
                                     device_id=pair, device_id_type=MESH).wait_send()

    @pl.when(cp < 2)
    def _():
        kv_sent(1)
        pltpu.make_async_remote_copy(relay_buf, relay_buf, relay_sem.at[1], relay_sem.at[0], device_id=across, device_id_type=MESH).wait_send()

    @pl.when(lax.rem(cp, 2) == 0)
    def _():
        kv_sent(0)

    @pl.when(cp >= 2)
    def _():
        kv_sent(2)


def fused_layer(tab, attn_gain, mlp_gain, x, w_q, w_k, w_v, w_o, w_gate, w_up, w_down):
    tok, width = x.shape
    qcols, kcols, ff = w_q.shape[1], w_k.shape[1], w_gate.shape[1]
    n_blk, n_kv, halves = width // BLK, kcols // HEAD_DIM, tok // HALF
    stacked = CHUNK * (qcols // kcols)
    dma = pltpu.SemaphoreType.DMA
    return pl.pallas_call(
        layer_kernel,
        in_specs=[ANY] * 11,
        out_specs=[VMEM] * 3,
        out_shape=[pltpu.VMEM((tok, width), BF)] + [pltpu.VMEM((tok, n_kv, HEAD_DIM), BF)] * 2,
        scratch_shapes=[
            pltpu.VMEM((N_SLOT * SLOT, BLK), BF),
            pltpu.VMEM((n_blk, tok, BLK), BF), pltpu.VMEM((n_blk, tok, BLK), BF), pltpu.VMEM((N_RELAY, UNIT, BLK), BF),
            pltpu.VMEM((tok, width), BF), pltpu.VMEM((HALF, ff), BF),
            pltpu.VMEM((4, n_kv, tok, 2 * HEAD_DIM), BF), pltpu.VMEM((tok, qcols), BF), pltpu.VMEM((CHUNK, qcols), BF),
            pltpu.VMEM((width // LANES, LANES), BF), pltpu.VMEM((width // LANES, LANES), BF),
            pltpu.VMEM((tok, HEAD_DIM), F32), pltpu.VMEM((tok, HEAD_DIM), F32), pltpu.VMEM((tok, HEAD_DIM), F32),
            pltpu.VMEM((2, 1, stacked), F32), pltpu.VMEM((2, 1, stacked), F32), pltpu.VMEM((2, HEAD_DIM, stacked), F32),
            dma((3,)), dma((tok // X_ROWS,)), dma((n_kv // 2, 2, KV_PARTS)), dma((N_SLOT,)), dma((3,)), dma((4, n_kv)),
            dma((halves,)), dma((halves,)), dma((halves,)), dma((halves, n_blk)), dma((2,)),
            pltpu.SemaphoreType.REGULAR((halves,))],
        compiler_params=pltpu.CompilerParams(vmem_limit_bytes=VMEM_LIMIT, collective_id=0, has_side_effects=True),
        name='fused_layer',
        cost_estimate=pl.CostEstimate(flops=2 * tok * width * (2 * qcols + 2 * kcols + 3 * ff), transcendentals=0,
                                      bytes_accessed=2 * width * (2 * qcols + 2 * kcols + 6 * ff)),
    )(tab, attn_gain, mlp_gain, x, w_q, w_k, w_v, w_o, w_gate, w_up, w_down)


def emit_kernel(y_ref, k_ref, v_ref, x_out, k_out, v_out, sem):
    copies = [pltpu.make_async_copy(y_ref.at[at(i, EMIT_ROWS), :], x_out.at[at(i, EMIT_ROWS), :], sem.at[i]) for i in range(y_ref.shape[0] // EMIT_ROWS)]
    copies += [pltpu.make_async_copy(k_ref, k_out, sem.at[len(copies)]), pltpu.make_async_copy(v_ref, v_out, sem.at[len(copies) + 1])]
    for c in copies:
        c.start()
    for c in copies:
        c.wait()


def emit(*results):
    here = [pltpu.with_memory_space_constraint(r, pltpu.VMEM) for r in results]
    return pl.pallas_call(
        emit_kernel, in_specs=[VMEM] * 3, out_specs=[ANY] * 3,
        out_shape=[jax.ShapeDtypeStruct(r.shape, r.dtype) for r in results],
        scratch_shapes=[pltpu.SemaphoreType.DMA((results[0].shape[0] // EMIT_ROWS + 2,))],
        compiler_params=pltpu.CompilerParams(vmem_limit_bytes=1 << 20), name='emit',
    )(*here)


def solution(mesh):
    row_spec = P(('dp', 'cp'), None)
    cache_spec = P(('dp', 'cp'), 'tp', None)
    col_spec = P(None, 'tp')
    split_rows = P('tp', None)
    vec_spec = P(None)

    def local_layer(x, attn_gain, w_q, w_k, w_v, w_o, mlp_gain, w_gate, w_up, w_down):
        tok, width = x.shape
        tab = jnp.asarray(rope_table(tok * mesh.shape['cp']))
        gains = [g.reshape(width // LANES, LANES) for g in (attn_gain, mlp_gain)]
        return tuple(emit(*fused_layer(tab, *gains, x, w_q, w_k, w_v, w_o, w_gate, w_up, w_down)))

    return jax.shard_map(local_layer, mesh=mesh,
                         in_specs=(row_spec, vec_spec, col_spec, col_spec, col_spec, split_rows, vec_spec, col_spec, col_spec, split_rows),
                         out_specs=(row_spec, cache_spec, cache_spec), check_vma=False)
```

```python
import jax
import jax.numpy as jnp
import numpy as np
from jax import lax
from jax.experimental import pallas as pl
from jax.experimental.pallas import tpu as pltpu
from jax.sharding import PartitionSpec as P

HEAD_DIM = 128
ROPE_THETA = 1000000.0
NORM_EPS = 1e-5
MASK_VALUE = -1e30
EXP2_SCALE = HEAD_DIM ** -0.5 * 1.4426950408889634
BF = jnp.bfloat16
F32 = jnp.float32
ANY = pl.BlockSpec(memory_space=pl.ANY)
VMEM = pl.BlockSpec(memory_space=pltpu.VMEM)
MESH = pl.DeviceIdType.MESH
LANES = 128
CHUNK = 128
HALF = 256
BLK = 512
SLOT = 2048
X_ROWS = 64
KV_ROWS = 128
N_RELAY = 5
UNIT = 64
KV_PARTS = 2
N_SLOT = 12
VMEM_LIMIT = 60000000
EMIT_ROWS = 512


def at(i, size):
    return pl.ds(pl.multiple_of(i * size, size), size)


def loop(n, body):
    def step(i, c):
        body(i)
        return c
    lax.fori_loop(0, n, step, 0)


def rope_table(n_pos):
    inv_freq = np.float32(ROPE_THETA) ** (-np.arange(0, HEAD_DIM, 2, dtype=np.float32) / np.float32(HEAD_DIM))
    angles = np.arange(n_pos, dtype=np.float32)[:, None] * inv_freq[None, :]
    return np.concatenate([np.cos(angles), np.sin(angles)], axis=1).astype(np.float32)


def layer_kernel(tab_ref, again_ref, mgain_ref, x_ref, wq_ref, wk_ref, wv_ref, wo_ref, wg_ref, wu_ref, wd_ref,
                 h_buf, k_out, v_out,
                 ring, send_buf, recv_buf, relay_buf, n_buf, act_buf, kv_buf, q_buf, o_buf, again_buf, mgain_buf, tab_buf, cos_buf, sin_buf, m_sc, l_sc, acc_sc,
                 tab_sem, x_sem, wkv_sem, w_sem, kvs_sem, kvr_sem, ps_sem, pr_sem, ds_sem, dr_sem, relay_sem, free_sem):
    cp = lax.axis_index('cp')
    peer = {'tp': 1 - lax.axis_index('tp')}
    pair = {'cp': cp + 1 - 2 * lax.rem(cp, 2)}
    across = {'cp': lax.rem(cp + 2, 4)}
    diagonal = {'tp': 1 - lax.axis_index('tp'), 'cp': lax.rem(cp + 2, 4)}
    tok, width = n_buf.shape
    n_blk = width // BLK
    n_gu = wg_ref.shape[1] // BLK
    n_q = wq_ref.shape[1] // BLK
    n_kv = wk_ref.shape[1] // HEAD_DIM
    groups = wq_ref.shape[1] // wk_ref.shape[1]
    n_chunk = tok // CHUNK
    stacked = groups * CHUNK
    gu_slots, d_slots = width // SLOT, wd_ref.shape[0] // SLOT
    gu_deep, d_deep = N_SLOT // (2 * gu_slots), N_SLOT // d_slots
    kv_slots = n_kv // 2 * gu_slots

    def ring_rows(slot, n):
        return pl.ds(pl.multiple_of(slot * SLOT, SLOT), n * SLOT)

    def load(src, slot, n):
        return pltpu.make_async_copy(src, ring.at[ring_rows(slot, n), :], w_sem.at[slot])

    def load_q(u):
        return load(wq_ref.at[:, at(u, BLK)], kv_slots + gu_slots * u, gu_slots)

    def wo_slot(t):
        return jnp.where(t < n_blk, lax.rem(t, kv_slots), lax.rem(t, N_SLOT))

    def load_wo(t):
        return load(wo_ref.at[:, at(lax.rem(t, n_blk), BLK)], wo_slot(t), 1)

    def gate_slot(j):
        return lax.rem(j, gu_deep) * 2 * gu_slots

    def load_gate(j):
        return load(wg_ref.at[:, at(j, BLK)], gate_slot(j), gu_slots)

    def load_up(j):
        return load(wu_ref.at[:, at(j, BLK)], gate_slot(j) + gu_slots, gu_slots)

    def load_down(j):
        return load(wd_ref.at[:, at(j, BLK)], lax.rem(j, d_deep) * d_slots, d_slots)

    def load_kv(u, which, part):
        src = (wk_ref, wv_ref)[which]
        n = width // KV_PARTS
        rows = pl.ds(part * n, n)
        dst = ring.at[pl.ds(u * gu_slots * SLOT + part * n, n), pl.ds(which * 2 * HEAD_DIM, 2 * HEAD_DIM)]
        return pltpu.make_async_copy(src.at[rows, pl.ds(u * 2 * HEAD_DIM, 2 * HEAD_DIM)], dst, wkv_sem.at[u, which, part])

    def all_kv(u):
        return [load_kv(u, which, part) for part in range(KV_PARTS) for which in range(2)]

    def load_x(i):
        return pltpu.make_async_copy(x_ref.at[at(i, X_ROWS), :], h_buf.at[at(i, X_ROWS), :], x_sem.at[i])

    def kv_copy(kind, g, r=0, n_rows=None):
        n_rows = n_rows or tok
        src_block = 2 if kind == 2 else 0
        rows = at(r, n_rows) if n_rows < tok else slice(None)
        return pltpu.make_async_remote_copy(kv_buf.at[src_block, g, rows, :], kv_buf.at[kind + 1, g, rows, :],
                                            kvs_sem.at[kind], kvr_sem.at[kind, g],
                                            device_id=across if kind == 1 else pair, device_id_type=MESH)

    def kv_half(kind, g, r):
        src_block = 2 if kind == 2 else 0
        rows = pl.ds(r * HALF, HALF)
        return pltpu.make_async_remote_copy(kv_buf.at[src_block, g, rows, :], kv_buf.at[kind + 1, g, rows, :],
                                            kvs_sem.at[kind], kvr_sem.at[kind if kind == 2 or r == 0 else 3, g],
                                            device_id=across if kind == 1 else pair, device_id_type=MESH)

    def part_copy(i, j):
        piece = (j, at(i, CHUNK), slice(None))
        return pltpu.make_async_remote_copy(send_buf.at[piece], recv_buf.at[piece], ps_sem.at[i * CHUNK // HALF], pr_sem.at[i * CHUNK // HALF],
                                            device_id=peer, device_id_type=MESH)

    per_piece = CHUNK // UNIT
    first_relay = n_blk * per_piece - N_RELAY

    def unit(g):
        return (g // per_piece, at(lax.rem(g, per_piece), UNIT), slice(None))

    def unit_copy(g):
        return pltpu.make_async_remote_copy(send_buf.at[unit(g)], recv_buf.at[unit(g)], ps_sem.at[0], pr_sem.at[0],
                                            device_id=peer, device_id_type=MESH)

    def relay_copy(g):
        return pltpu.make_async_remote_copy(send_buf.at[unit(g)], relay_buf.at[g - first_relay], ps_sem.at[0], relay_sem.at[0],
                                            device_id=diagonal, device_id_type=MESH)

    def forward_copy(g):
        return pltpu.make_async_remote_copy(relay_buf.at[g - first_relay], recv_buf.at[unit(g)], relay_sem.at[1], pr_sem.at[0],
                                            device_id=across, device_id_type=MESH)

    def down_copy(s, j):
        piece = (j, at(s, HALF), slice(None))
        return pltpu.make_async_remote_copy(send_buf.at[piece], recv_buf.at[piece], ds_sem.at[s], dr_sem.at[s, j],
                                            device_id=peer, device_id_type=MESH)

    def half_copy(s, sent_sem, got_sem):
        piece = (slice(None), at(s, HALF), slice(None))
        return pltpu.make_async_remote_copy(send_buf.at[piece], recv_buf.at[piece], sent_sem.at[s], got_sem,
                                            device_id=peer, device_id_type=MESH)

    def scale_rows(src_rows, dst_rows, total, gain_ref):
        inv = lax.rsqrt(jnp.sum(total, axis=-1, keepdims=True) / width + NORM_EPS)
        for r in range(width // LANES):
            cols = slice(r * LANES, (r + 1) * LANES)
            wide = h_buf[src_rows, cols].astype(F32)
            n_buf[dst_rows, cols] = (wide * inv * gain_ref[r:r + 1, :].astype(F32)).astype(BF)

    def rope(prod, rows):
        u = prod.astype(BF).astype(F32)
        return (u * cos_buf[rows, :] + pltpu.roll(u, HEAD_DIM // 2, 1) * sin_buf[rows, :]).astype(BF)

    barrier = pltpu.get_barrier_semaphore()
    for other in (peer, pair, across, diagonal):
        pl.semaphore_signal(barrier, inc=1, device_id=other, device_id_type=MESH)

    gain_copy = pltpu.make_async_copy(again_ref, again_buf, tab_sem.at[0])
    small = [pltpu.make_async_copy(mgain_ref, mgain_buf, tab_sem.at[1]), pltpu.make_async_copy(tab_ref.at[at(cp, tok), :], tab_buf, tab_sem.at[2])]
    gain_copy.start()
    first_rows = KV_ROWS // X_ROWS
    loop(first_rows, lambda i: load_x(i).start())
    for c in all_kv(0) + small:
        c.start()
    lax.fori_loop(first_rows, tok // X_ROWS, lambda i, c: (load_x(i).start(), c)[1], 0)
    gain_copy.wait()

    def norm_step(i):
        load_x(i).wait()
        for part in range(X_ROWS // 32):
            rows = at(i * (X_ROWS // 32) + part, 32)
            total = jnp.zeros((32, BLK), F32)
            for j in range(n_blk):
                wide = h_buf[rows, j * BLK:(j + 1) * BLK].astype(F32)
                total += wide * wide
            scale_rows(rows, rows, total, again_buf)

    n_quarter = tok // KV_ROWS

    def send_kv(*piece):
        @pl.when(cp < 2)
        def _():
            if len(piece) == 1 and piece[0] % 2:
                for r in range(tok // HALF):
                    kv_half(1, piece[0], r).start()
            else:
                kv_copy(1, *piece).start()

        @pl.when(lax.rem(cp, 2) == 0)
        def _():
            kv_copy(0, *piece).start()

    def kv_rows(u, rows, before_rope=None):
        prod = jnp.dot(n_buf[rows, :], ring[ring_rows(u * gu_slots, gu_slots), :], preferred_element_type=F32)
        if before_rope is not None:
            before_rope()
        for e in range(2):
            kv_buf[0, 2 * u + e, rows, :HEAD_DIM] = rope(prod[:, e * HEAD_DIM:(e + 1) * HEAD_DIM], rows)
            kv_buf[0, 2 * u + e, rows, HEAD_DIM:] = prod[:, (e + 2) * HEAD_DIM:(e + 3) * HEAD_DIM].astype(BF)

    def build_tables(r):
        @pl.when(r == 0)
        def _():
            for c in small:
                c.wait()
            cos, sin = tab_buf[:, :HEAD_DIM // 2], tab_buf[:, HEAD_DIM // 2:]
            cos_buf[...] = jnp.concatenate([cos, cos], axis=1)
            sin_buf[...] = jnp.concatenate([-sin, sin], axis=1)

    def kv_step(r):
        lax.fori_loop(r * (KV_ROWS // X_ROWS), (r + 1) * (KV_ROWS // X_ROWS), lambda i, c: (norm_step(i), c)[1], 0)

        @pl.when(r == 0)
        def _():
            for c in all_kv(0):
                c.wait()

        @pl.when(r == 1)
        def _():
            for u in range(1, n_kv // 2):
                for c in all_kv(u):
                    c.start()
            for u in range(n_q):
                load_q(u).start()
        kv_rows(0, at(r, KV_ROWS), lambda: build_tables(r))

        @pl.when(r == 0)
        def _():
            pl.semaphore_wait(barrier, 4)
        send_kv(0, r, KV_ROWS)
    loop(n_quarter, kv_step)
    send_kv(1)
    for u in range(1, n_kv // 2):
        for c in all_kv(u):
            c.wait()
        kv_rows(u, slice(None))
        send_kv(2 * u)
        send_kv(2 * u + 1)
    for t in range(kv_slots):
        load_wo(t).start()

    def q_rows(u, row, n):
        w = ring[ring_rows(kv_slots + gu_slots * u, gu_slots), :]
        prod = jnp.dot(n_buf[row:row + n, :], w, preferred_element_type=F32)
        for j in range(BLK // HEAD_DIM):
            cols = pl.ds(pl.multiple_of(u * BLK + j * HEAD_DIM, HEAD_DIM), HEAD_DIM)
            q_buf[row:row + n, cols] = rope(prod[:, j * HEAD_DIM:(j + 1) * HEAD_DIM], slice(row, row + n))

    def q_first(u):
        load_q(u).wait()
        q_rows(u, 0, CHUNK)
    loop(n_q, q_first)

    def q_rest(u, c):
        q_rows(u, CHUNK, tok - CHUNK)
        for e in range(gu_slots):
            t = kv_slots + gu_slots * u + e
            load_wo(jnp.where(t < n_blk, t + N_SLOT, t)).start()
        return c
    q_early = jnp.where(cp >= 2, n_q - 2, 0)

    lo = jnp.where(cp == 2, 2, 1)
    hi = jnp.where(cp == 0, 1, jnp.where(cp == 1, 2, 4))
    for i in range(n_chunk):
        row0 = i * CHUNK
        n_keys = row0 + CHUNK

        n_heads = 2

        def scores(g, b, n):
            q = jnp.concatenate([q_buf[row0:row0 + CHUNK, at(g * groups + j, HEAD_DIM)] for j in range(groups)], axis=0)
            return lax.dot_general(kv_buf[b, g, :n, :HEAD_DIM], q, (((1,), (1,)), ((), ())), preferred_element_type=F32)

        def weigh(g, b, n, p):
            return lax.dot_general(kv_buf[b, g, :n, HEAD_DIM:], p.astype(BF), (((0,), (0,)), ((), ())), preferred_element_type=F32)

        def pass_on(g):
            kv_copy(1, g).wait_recv()
            kv_copy(2, g).start()

        def head_step(step):
            heads = [step * n_heads + e for e in range(n_heads)]
            kpos = lax.broadcasted_iota(jnp.int32, (n_keys, stacked), 0)
            qpos = row0 + lax.rem(lax.broadcasted_iota(jnp.int32, (n_keys, stacked), 1), CHUNK)
            if i == 0:
                @pl.when(cp >= 2)
                def _():
                    pass_on(heads[0])
            all_s = [scores(g, 0, n_keys) for g in heads]
            for e, g in enumerate(heads):
                s = jnp.where(kpos <= qpos, all_s[e], MASK_VALUE)
                m0 = jnp.max(s, axis=0, keepdims=True)
                p = jnp.exp2(s * EXP2_SCALE - m0 * EXP2_SCALE)
                m_sc[e] = m0
                l_sc[e] = jnp.sum(p, axis=0, keepdims=True)
                acc_sc[e] = weigh(g, 0, n_keys, p)

            def block_step(b, c):
                if i == 0:
                    @pl.when(b == 1)
                    def _():
                        for g in heads:
                            kv_copy(0, g).wait_recv()

                    @pl.when(b == 2)
                    def _():
                        for r in range(tok // HALF):
                            kv_half(1, heads[1], r).wait_recv()
                            kv_half(2, heads[1], r).start()

                    @pl.when(b == 3)
                    def _():
                        for g in heads:
                            kv_copy(2, g).wait_recv()
                all_s = [scores(g, b, tok) for g in heads]
                for e, g in enumerate(heads):
                    s = all_s[e]
                    m_old = m_sc[e]
                    m_new = jnp.maximum(m_old, jnp.max(s, axis=0, keepdims=True))
                    alpha = jnp.exp2((m_old - m_new) * EXP2_SCALE)
                    p = jnp.exp2(s * EXP2_SCALE - m_new * EXP2_SCALE)
                    l_sc[e] = l_sc[e] * alpha + jnp.sum(p, axis=0, keepdims=True)
                    acc_sc[e] = acc_sc[e] * alpha + weigh(g, b, tok, p)
                    m_sc[e] = m_new
                return c
            lax.fori_loop(lo, hi, block_step, 0)
            for e, g in enumerate(heads):
                out = acc_sc[e] / l_sc[e]
                for j in range(groups):
                    o_buf[:, at(g * groups + j, HEAD_DIM)] = out[:, j * CHUNK:(j + 1) * CHUNK].T.astype(BF)
            if i == 0:
                lax.fori_loop(jnp.where(step == 0, 0, q_early), q_early, q_rest, 0)
        loop(n_kv // n_heads, head_step)

        def wo_step(j):
            t = i * n_blk + j
            load_wo(t).wait()
            w = ring[ring_rows(wo_slot(t), 1), :]
            send_buf[j, row0:row0 + CHUNK, :] = jnp.dot(o_buf[...], w, preferred_element_type=F32).astype(BF)
            if i > 0:
                part_copy(i, j).start()
            else:
                @pl.when(cp < 2)
                def _():
                    part_copy(i, j).start()

                for e in range(per_piece):
                    g = j * per_piece + e

                    @pl.when((cp >= 2) & (g < first_relay))
                    def _():
                        unit_copy(g).start()

                    @pl.when((cp >= 2) & (g >= first_relay))
                    def _():
                        relay_copy(g).start()
            if i == 0:
                load_wo(jnp.where(j < kv_slots, t + kv_slots, t + n_blk)).start()
            elif (i + 1) * n_blk - 1 + N_SLOT < n_chunk * n_blk:
                load_wo(t + N_SLOT).start()
            else:
                @pl.when(t + N_SLOT < n_chunk * n_blk)
                def _():
                    load_wo(t + N_SLOT).start()

                first = n_chunk * n_blk - N_SLOT
                for b in range(gu_deep):
                    end = 2 * gu_slots * b
                    for which in range(2):
                        last_slot = end + which * gu_slots + gu_slots - 1
                        when = first + (last_slot - first) % N_SLOT

                        @pl.when(t == when)
                        def _():
                            (load_gate, load_up)[which](b).start()
        loop(n_blk, wo_step)
        if i == 0:
            lax.fori_loop(q_early, n_q, q_rest, 0)

    def half_step(s):
        @pl.when((s == 0) & (cp < 2))
        def _():
            pltpu.make_async_remote_copy(relay_buf, relay_buf, relay_sem.at[1], relay_sem.at[0], device_id=across, device_id_type=MESH).wait_recv()
            loop(N_RELAY, lambda k: forward_copy(first_relay + k).start())
        parts = half_copy(s, ps_sem, pr_sem.at[s])
        parts.wait_recv()
        parts.wait_send()

        def h_step(r):
            rows = at(s * (HALF // 32) + r, 32)
            total = jnp.zeros((32, BLK), F32)
            for j in range(n_blk):
                cols = slice(j * BLK, (j + 1) * BLK)
                add = send_buf[j, rows, :].astype(F32) + recv_buf[j, rows, :].astype(F32)
                h = (h_buf[rows, cols].astype(F32) + add).astype(BF)
                h_buf[rows, cols] = h
                wide = h.astype(F32)
                total += wide * wide
            scale_rows(rows, at(r, 32), total, mgain_buf)
        loop(HALF // 32, h_step)
        pl.semaphore_signal(free_sem.at[s], inc=1, device_id=peer, device_id_type=MESH)

        def gu_step(j):
            slot = gate_slot(j)
            load_gate(j).wait()
            gate = jnp.dot(n_buf[:HALF, :], ring[ring_rows(slot, gu_slots), :], preferred_element_type=F32)
            load_up(j).wait()
            up = jnp.dot(n_buf[:HALF, :], ring[ring_rows(slot + gu_slots, gu_slots), :], preferred_element_type=F32)
            act_buf[:, at(j, BLK)] = (gate / (1.0 + jnp.exp(-gate)) * up).astype(BF)

            @pl.when(j + gu_deep < n_gu)
            def _():
                load_gate(j + gu_deep).start()
                load_up(j + gu_deep).start()
            freed = 0
            for back in range(gu_deep, 0, -1):
                now = (2 * gu_slots * (gu_deep - back + 1)) // d_slots

                @pl.when(j == n_gu - back)
                def _():
                    for d in range(freed, now):
                        load_down(d).start()
                freed = now
        loop(n_gu, gu_step)
        pl.semaphore_wait(free_sem.at[s], 1)

        def down_step(j):
            load_down(j).wait()
            w = ring[ring_rows(lax.rem(j, d_deep) * d_slots, d_slots), :]
            send_buf[j, at(s, HALF), :] = jnp.dot(act_buf[...], w, preferred_element_type=F32).astype(BF)
            down_copy(s, j).start()

            @pl.when(j + d_deep < n_blk)
            def _():
                load_down(j + d_deep).start()
            freed = 0
            for back in range(d_deep, 0, -1):
                now = d_slots * (d_deep - back + 1) // gu_slots

                @pl.when((j == n_blk - back) & (s == 0))
                def _():
                    for d in range(freed, now):
                        (load_gate, load_up)[d % 2](d // 2).start()
                freed = now
        loop(n_blk, down_step)
    loop(tok // HALF, half_step)

    for g in range(n_kv):
        k_out[:, g, :] = kv_buf[0, g, :, :HEAD_DIM]
        v_out[:, g, :] = kv_buf[0, g, :, HEAD_DIM:]

    def final_step(t):
        s, j = t // n_blk, lax.rem(t, n_blk)
        down_copy(s, j).wait_recv()
        rows, cols = at(s, HALF), at(j, BLK)
        add = send_buf[j, rows, :].astype(F32) + recv_buf[j, rows, :].astype(F32)
        h_buf[rows, cols] = (h_buf[rows, cols].astype(F32) + add).astype(BF)
    loop(tok // HALF * n_blk, final_step)

    loop(tok // HALF, lambda s: half_copy(s, ds_sem, pr_sem.at[s]).wait_send())
    def kv_sent(kind):
        pltpu.make_async_remote_copy(kv_buf.at[0], kv_buf.at[kind + 1], kvs_sem.at[kind], kvr_sem.at[kind, 0],
                                     device_id=pair, device_id_type=MESH).wait_send()

    @pl.when(cp < 2)
    def _():
        kv_sent(1)
        pltpu.make_async_remote_copy(relay_buf, relay_buf, relay_sem.at[1], relay_sem.at[0], device_id=across, device_id_type=MESH).wait_send()

    @pl.when(lax.rem(cp, 2) == 0)
    def _():
        kv_sent(0)

    @pl.when(cp >= 2)
    def _():
        kv_sent(2)


def fused_layer(tab, attn_gain, mlp_gain, x, w_q, w_k, w_v, w_o, w_gate, w_up, w_down):
    tok, width = x.shape
    qcols, kcols, ff = w_q.shape[1], w_k.shape[1], w_gate.shape[1]
    n_blk, n_kv, halves = width // BLK, kcols // HEAD_DIM, tok // HALF
    stacked = CHUNK * (qcols // kcols)
    dma = pltpu.SemaphoreType.DMA
    return pl.pallas_call(
        layer_kernel,
        in_specs=[ANY] * 11,
        out_specs=[VMEM] * 3,
        out_shape=[pltpu.VMEM((tok, width), BF)] + [pltpu.VMEM((tok, n_kv, HEAD_DIM), BF)] * 2,
        scratch_shapes=[
            pltpu.VMEM((N_SLOT * SLOT, BLK), BF),
            pltpu.VMEM((n_blk, tok, BLK), BF), pltpu.VMEM((n_blk, tok, BLK), BF), pltpu.VMEM((N_RELAY, UNIT, BLK), BF),
            pltpu.VMEM((tok, width), BF), pltpu.VMEM((HALF, ff), BF),
            pltpu.VMEM((4, n_kv, tok, 2 * HEAD_DIM), BF), pltpu.VMEM((tok, qcols), BF), pltpu.VMEM((CHUNK, qcols), BF),
            pltpu.VMEM((width // LANES, LANES), BF), pltpu.VMEM((width // LANES, LANES), BF),
            pltpu.VMEM((tok, HEAD_DIM), F32), pltpu.VMEM((tok, HEAD_DIM), F32), pltpu.VMEM((tok, HEAD_DIM), F32),
            pltpu.VMEM((2, 1, stacked), F32), pltpu.VMEM((2, 1, stacked), F32), pltpu.VMEM((2, HEAD_DIM, stacked), F32),
            dma((3,)), dma((tok // X_ROWS,)), dma((n_kv // 2, 2, KV_PARTS)), dma((N_SLOT,)), dma((3,)), dma((4, n_kv)),
            dma((halves,)), dma((halves,)), dma((halves,)), dma((halves, n_blk)), dma((2,)),
            pltpu.SemaphoreType.REGULAR((halves,))],
        compiler_params=pltpu.CompilerParams(vmem_limit_bytes=VMEM_LIMIT, collective_id=0, has_side_effects=True),
        name='fused_layer',
        cost_estimate=pl.CostEstimate(flops=2 * tok * width * (2 * qcols + 2 * kcols + 3 * ff), transcendentals=0,
                                      bytes_accessed=2 * width * (2 * qcols + 2 * kcols + 6 * ff)),
    )(tab, attn_gain, mlp_gain, x, w_q, w_k, w_v, w_o, w_gate, w_up, w_down)


def emit_kernel(y_ref, k_ref, v_ref, x_out, k_out, v_out, sem):
    copies = [pltpu.make_async_copy(y_ref.at[at(i, EMIT_ROWS), :], x_out.at[at(i, EMIT_ROWS), :], sem.at[i]) for i in range(y_ref.shape[0] // EMIT_ROWS)]
    copies += [pltpu.make_async_copy(k_ref, k_out, sem.at[len(copies)]), pltpu.make_async_copy(v_ref, v_out, sem.at[len(copies) + 1])]
    for c in copies:
        c.start()
    for c in copies:
        c.wait()


def emit(*results):
    here = [pltpu.with_memory_space_constraint(r, pltpu.VMEM) for r in results]
    return pl.pallas_call(
        emit_kernel, in_specs=[VMEM] * 3, out_specs=[ANY] * 3,
        out_shape=[jax.ShapeDtypeStruct(r.shape, r.dtype) for r in results],
        scratch_shapes=[pltpu.SemaphoreType.DMA((results[0].shape[0] // EMIT_ROWS + 2,))],
        compiler_params=pltpu.CompilerParams(vmem_limit_bytes=1 << 20), name='emit',
    )(*here)


def solution(mesh):
    row_spec = P(('dp', 'cp'), None)
    cache_spec = P(('dp', 'cp'), 'tp', None)
    col_spec = P(None, 'tp')
    split_rows = P('tp', None)
    vec_spec = P(None)

    def local_layer(x, attn_gain, w_q, w_k, w_v, w_o, mlp_gain, w_gate, w_up, w_down):
        tok, width = x.shape
        tab = jnp.asarray(rope_table(tok * mesh.shape['cp']))
        gains = [g.reshape(width // LANES, LANES) for g in (attn_gain, mlp_gain)]
        return tuple(emit(*fused_layer(tab, *gains, x, w_q, w_k, w_v, w_o, w_gate, w_up, w_down)))

    return jax.shard_map(local_layer, mesh=mesh,
                         in_specs=(row_spec, vec_spec, col_spec, col_spec, col_spec, split_rows, vec_spec, col_spec, col_spec, split_rows),
                         out_specs=(row_spec, cache_spec, cache_spec), check_vma=False)
```
